32 devices in a mesh: group: 2 (over y), dev: 16 (over z, x, core).
Axes of the slice: x: 2, y: 2, z: 4, core: 2. Of those that a mesh axis runs over, the one named last changes fastest.
Arguments:
- bin_index: int32 [131072, 128], P(('group', 'dev')), may hold values from 0 to 63
- gradient: bfloat16 [131072], P(('group', 'dev')), may hold values from -6 to 6
- hessian: bfloat16 [131072], P(('group', 'dev')), may hold values from 0.049804688 to 0.25
- child_id: int32 [131072], P(('group', 'dev')), may hold values from 0 to 63
- smaller_side: int32 [32], replicated, may hold values from 0 to 1
Outputs:
- best_gain: float32 [32, 128], P('group', 'dev')
- child_best: float32 [32], P('group')
The draws below stay inside these ranges and needn't reach their ends.
All inputs are finite; a program needn't handle non-finite values.
Results may differ from the reference program's by a relative error of at most 0.0003.
Values sent between devices are 32-bit elements; how exact they have to be, the bound alone decides.
A program may use at most 64 MiB of HBM per device.

```python
import math
import jax
import jax.numpy as jnp
from jax import lax

FEAT = 128
BINS = 64
PAIRS = 32
ROWS = 131072


def place_ends(values, own_key, least, largest):
    spot = [jax.random.randint(jax.random.fold_in(own_key, axis), (), 0, length) for axis, length in enumerate(values.shape)]
    main_axis = values.shape.index(max(values.shape))
    beside = spot[:main_axis] + [(spot[main_axis] + 1) % values.shape[main_axis]] + spot[main_axis + 1:]
    return values.at[tuple(spot)].set(least).at[tuple(beside)].set(largest)


def shard_levels(own_key, extent, cuts, low, top_value):
    loudness = 1.0
    for position, parts in cuts:
        draws = jax.random.uniform(jax.random.fold_in(jax.random.fold_in(own_key, 6), position), (parts,), jnp.float32, low / len(cuts), top_value / len(cuts))
        loudness = loudness * jnp.repeat(jnp.exp(draws), extent[position] // parts).reshape((-1,) + (1,) * (len(extent) - 1 - position))
    return loudness


def gaussian(own_key, extent, deviation, reach, cuts=(), kind=jnp.bfloat16):
    result = deviation * jax.random.normal(own_key, extent, jnp.float32)
    if cuts:
        result = result * shard_levels(own_key, extent, cuts, -0.22, 0.18)
    return jnp.clip(result, -reach, reach).astype(kind)


def setup_inputs(seed: int = 0) -> dict:
    key_list = jax.random.split(jax.random.key(seed), 6)
    return {
        "bin_index": place_ends(jax.random.randint(key_list[0], (ROWS, FEAT), 0, BINS), jax.random.fold_in(key_list[0], 1), 0, BINS - 1).astype(jnp.int32),
        "gradient": gaussian(key_list[1], (ROWS,), 1.0, 6.0, ((0, 32),)),
        "hessian": jnp.clip(0.049804688 + 0.20019531 * jax.random.uniform(key_list[2], (ROWS,), jnp.float32) ** shard_levels(key_list[2], (ROWS,), ((0, 32),), -0.2, 0.2), 0.049804688, 0.25).astype(jnp.bfloat16),
        "child_id": place_ends(jax.random.randint(key_list[3], (ROWS,), 0, 2 * PAIRS), jax.random.fold_in(key_list[3], 1), 0, (2 * PAIRS) - 1).astype(jnp.int32),
        "smaller_side": place_ends(jax.random.randint(key_list[4], (PAIRS,), 0, 2), jax.random.fold_in(key_list[4], 1), 0, 1).astype(jnp.int32),
    }


reg_lambda = 1.0


def split_gains(hist_grad, hist_hess):
    left_grad = jnp.cumsum(hist_grad, axis=-1)[..., :-1]
    left_hess = jnp.cumsum(hist_hess, axis=-1)[..., :-1]
    total_grad = jnp.sum(hist_grad, axis=-1, keepdims=True)
    total_hess = jnp.sum(hist_hess, axis=-1, keepdims=True)
    right_grad = total_grad - left_grad
    value = left_grad * left_grad / (left_hess + reg_lambda)
    value = value + right_grad * right_grad / (total_hess - left_hess + reg_lambda)
    value = value - total_grad * total_grad / (total_hess + reg_lambda)
    return jnp.max(value, axis=-1)


def reference(bin_index, gradient, hessian, child_id, smaller_side):
    row_count = bin_index.shape[0]
    pair_index = (child_id // 2).astype(jnp.int32)
    member = (child_id - 2 * pair_index == smaller_side[pair_index]).astype(jnp.float32)
    values = jnp.stack([gradient.astype(jnp.float32) * member, hessian.astype(jnp.float32) * member], axis=1)
    block_size = math.gcd(FEAT, 8)
    offsets = jnp.arange(block_size, dtype=jnp.int32) * (PAIRS * BINS)
    base_index = (pair_index * BINS).astype(jnp.int32)

    def one_block(number):
        columns = lax.dynamic_slice_in_dim(bin_index, (number * block_size).astype(jnp.int32), block_size, 1)
        segment = base_index[:, None] + columns + offsets[None, :]
        spread = jnp.broadcast_to(values[:, None, :], (row_count, block_size, 2))
        summed = jax.ops.segment_sum(spread.reshape(-1, 2), segment.reshape(-1).astype(jnp.int32), num_segments=block_size * PAIRS * BINS)
        return summed.reshape(block_size, PAIRS, BINS, 2)

    hist = lax.map(one_block, jnp.arange(FEAT // block_size, dtype=jnp.int32)).reshape(FEAT, PAIRS, BINS, 2)
    best_gain = split_gains(hist[..., 0], hist[..., 1]).T
    child_best = jnp.max(best_gain, axis=1)
    return best_gain, child_best
```

```python
import functools

import jax
import jax.numpy as jnp
from jax import lax
from jax.experimental import pallas as pl
from jax.experimental.pallas import tpu as pltpu
from jax.sharding import PartitionSpec as P

BINS = 64
LANES = 128
KCHUNK = 1024
STEP_ROWS = 512


reg_lambda = 1.0


def split_gains(hist_grad, hist_hess):
    left_grad = jnp.cumsum(hist_grad, axis=-1)[..., :-1]
    left_hess = jnp.cumsum(hist_hess, axis=-1)[..., :-1]
    total_grad = jnp.sum(hist_grad, axis=-1, keepdims=True)
    total_hess = jnp.sum(hist_hess, axis=-1, keepdims=True)
    right_grad = total_grad - left_grad
    value = left_grad * left_grad / (left_hess + reg_lambda)
    value = value + right_grad * right_grad / (total_hess - left_hess + reg_lambda)
    value = value - total_grad * total_grad / (total_hess + reg_lambda)
    return jnp.max(value, axis=-1)


def plain_body(bin_index, gradient, hessian, child_id, smaller_side):
    leaves = smaller_side.shape[0]
    features = bin_index.shape[1]
    target = 2 * jnp.arange(leaves, dtype=jnp.int32)[None, :] + smaller_side[None, :]
    chosen = child_id[:, None] == target
    nothing = jnp.zeros((), jnp.bfloat16)
    weights = jnp.concatenate(
        [
            jnp.where(chosen, gradient[:, None], nothing),
            jnp.where(chosen, hessian[:, None], nothing),
        ],
        axis=1,
    )
    levels = jnp.arange(BINS, dtype=jnp.int32)

    def one_feature(column):
        onehot = (column[:, None] == levels[None, :]).astype(jnp.bfloat16)
        product = lax.dot_general(
            weights, onehot, (((0,), (0,)), ((), ())), preferred_element_type=jnp.float32
        )
        return product.reshape(2, leaves, BINS).transpose(1, 0, 2).reshape(leaves, 2 * BINS)

    stacked = lax.map(one_feature, bin_index.T)
    owned = lax.psum_scatter(stacked, "dev", scatter_dimension=0, tiled=True)
    owned = lax.psum_scatter(owned, "group", scatter_dimension=1, tiled=True)
    hist_grad = owned[:, :, :BINS].transpose(1, 0, 2)
    hist_hess = owned[:, :, BINS:].transpose(1, 0, 2)
    best_gain = split_gains(hist_grad, hist_hess)
    child_best = lax.pmax(jnp.max(best_gain, axis=1), "dev")
    return (best_gain, child_best)


def kernel(
    groups, devs, leaves,
    bins_ref, grad_ref, hess_ref, child_ref, side_ref,
    done_ref,
    bins_v, side_v, grad_v, hess_v, child_v, values, bins_sem, small_sem,
    bins_t, weights, out, pair_in, a_in, b_in, c_in, d_in, e_in, f_out, f_in, near_in,
    gain_out, gain_in, best_in,
    pair_sem, a_sem, b_sem, c_sem, d_sem, e_sem, f_sem, near_sem, gain_sem, best_sem,
):
    rows, features = bins_ref.shape
    per_dev = features // devs
    own_features = per_dev // groups
    own_leaves = leaves // groups
    width = 2 * leaves
    slots = LANES // width
    quads = own_features // slots
    half = quads // 2
    planes = devs // 4
    last = planes - 1
    relayed = last - 1
    me_g = lax.axis_index("group")
    me_d = lax.axis_index("dev")
    me_c = lax.rem(me_d, 2)
    me_j = lax.div(me_d, 2)
    me_x = lax.rem(me_j, 2)
    me_z = lax.div(me_j, 2)
    barrier = pltpu.get_barrier_semaphore()
    step_rows = STEP_ROWS
    everyone = groups * devs

    def bins_copy(number):
        here = pl.ds(pl.multiple_of(number * step_rows, step_rows), step_rows)
        return pltpu.make_async_copy(bins_ref.at[here, :], bins_v.at[here, :], bins_sem.at[number])

    small = [
        pltpu.make_async_copy(source, place, small_sem.at[number])
        for number, (source, place) in enumerate(
            [(side_ref, side_v), (child_ref, child_v), (grad_ref, grad_v), (hess_ref, hess_v)]
        )
    ]
    for copy in small:
        copy.start()

    def start_bins(number, carry):
        bins_copy(number).start()
        return carry

    lax.fori_loop(0, rows // step_rows, start_bins, 0)

    def at(g, d):
        return {"group": g, "dev": d}

    def nth(step):
        other = lax.rem(me_g * devs + me_d + step, everyone)
        return at(lax.div(other, devs), lax.rem(other, devs))

    def greet(step, carry):
        pl.semaphore_signal(barrier, inc=1, device_id=nth(step), device_id_type=pl.DeviceIdType.MESH)
        return carry

    lax.fori_loop(1, everyone, greet, 0)

    pair_row = lax.broadcasted_iota(jnp.int32, (leaves, leaves), 0)
    pair_lane = lax.broadcasted_iota(jnp.int32, (leaves, leaves), 1)

    for copy in small:
        copy.wait()

    side = jnp.where(pair_lane == pair_row, side_v[...].astype(jnp.float32), 0.0)
    target = jnp.sum(side, axis=1, keepdims=True) + 2.0 * pair_row[:, :1].astype(jnp.float32)
    target = jnp.broadcast_to(target, (leaves, LANES)).astype(jnp.bfloat16)
    values[0] = grad_v[...].astype(jnp.float32)
    values[1] = hess_v[...].astype(jnp.float32)
    values[2] = child_v[...].astype(jnp.float32)
    no_weight = jnp.zeros((), jnp.bfloat16)

    def prepare(number, carry):
        here = pl.ds(pl.multiple_of(number * step_rows, step_rows), step_rows)
        for piece in range(step_rows // LANES):
            row = number * (step_rows // LANES) + piece
            there = pl.ds(pl.multiple_of(row * LANES, LANES), LANES)

            def spread(kind):
                return jnp.broadcast_to(values[kind, pl.ds(row, 1), :], (leaves, LANES)).astype(jnp.bfloat16)

            chosen = spread(2) == target
            for kind in range(2):
                value = jnp.where(chosen, spread(kind), no_weight)
                for s in range(slots):
                    start = s * width + kind * leaves
                    weights[start:start + leaves, there] = value
        bins_copy(number).wait()
        bins_t[:, here] = bins_v[here, :].astype(jnp.float32).T
        return carry

    lax.fori_loop(0, rows // step_rows, prepare, 0)

    chunk = min(rows, KCHUNK)
    pack = 16
    level = lax.broadcasted_iota(jnp.int32, (pack, chunk), 0).astype(jnp.float32).astype(jnp.bfloat16)
    one = jnp.ones((), jnp.bfloat16)
    zero = jnp.zeros((), jnp.bfloat16)
    lane = lax.broadcasted_iota(jnp.int32, (BINS, LANES), 1)

    def block(d):
        base = pl.multiple_of(d * per_dev, per_dev)
        total = None
        for start in range(0, rows, chunk):
            parts = []
            levels = bins_t[pl.ds(base, per_dev), start:start + chunk]
            for f in range(per_dev):
                row = jnp.broadcast_to(levels[f:f + 1, :], (pack, chunk)).astype(jnp.bfloat16)
                for low in range(0, BINS, pack):
                    parts.append(jnp.where(row <= level + jnp.bfloat16(low), one, zero))
            below = jnp.concatenate(parts, axis=0)
            product = lax.dot_general(
                below, weights[:, start:start + chunk], (((1,), (1,)), ((), ())),
                preferred_element_type=jnp.float32,
            )
            total = product if total is None else total + product
        result = []
        for y in range(groups):
            for q in range(quads):
                piece = None
                for s in range(slots):
                    f = (y * quads + q) * slots + s
                    here = total[f * BINS:(f + 1) * BINS, :]
                    piece = here if piece is None else jnp.where(lane >= s * width, here, piece)
                result.append((y, q, piece))
        return result

    def remote(source, place, sem, index, device):
        return pltpu.make_async_remote_copy(
            src_ref=source, dst_ref=place, send_sem=sem.at[0, index], recv_sem=sem.at[1, index],
            device_id=device, device_id_type=pl.DeviceIdType.MESH,
        )

    def pick(index, choices):
        result = choices[-1]
        for number in range(len(choices) - 1):
            result = jnp.where(index == number, choices[number], result)
        return result

    def flipped(turn):
        result, bit = 0, 1
        while bit < planes:
            digit = lax.rem(lax.div(me_z, bit), 2)
            result = result + bit * (1 - digit if (turn // bit) % 2 else digit)
            bit *= 2
        return result

    planes_of = [flipped(last - k) for k in range(planes)]

    def plane(k):
        return planes_of[k] if isinstance(k, int) else pick(k, planes_of)

    def dev_of(k, dx, core):
        x = jnp.where(dx == 1, 1 - me_x, me_x)
        return (plane(k) * 2 + x) * 2 + core

    pair_dev = at(me_g, me_j * 2 + 1 - me_c)
    x_dev_d = (me_z * 2 + 1 - me_x) * 2 + me_c
    x_dev = at(me_g, x_dev_d)
    y_g = 1 - me_g
    y_dev = at(y_g, me_d)
    diag_dev = at(y_g, x_dev_d)

    def pair_copy(n):
        return remote(out.at[0, n], pair_in.at[n], pair_sem, n, pair_dev)

    first = slice(0, half)
    second = slice(half, quads)

    def a_copy(k):
        return remote(out.at[1, 2 * k + 1, first], a_in.at[k], a_sem, k, x_dev)

    def b_copy(k):
        return remote(out.at[1, 2 * k + 1, second, me_g], b_in.at[k], b_sem, k, x_dev)

    def c_copy(k):
        return remote(out.at[1, 2 * k + 1, second, y_g], c_in.at[k], c_sem, k, y_dev)

    def d_copy(k):
        return remote(out.at[1, 2 * k, second, y_g], d_in.at[k], d_sem, k, y_dev)

    def e_copy(k):
        return remote(out.at[1, 2 * k, first, y_g], e_in.at[k], e_sem, k, y_dev)

    def f_copy(k):
        d = (plane(k) * 2 + me_x) * 2 + me_c
        return remote(f_out.at[k], f_in.at[k], f_sem, k, at(me_g, d))

    def direct_copy(k, n):
        dx, y = ((1, y_g), (1, me_g), (0, y_g), (0, me_g))[n]
        d = dev_of(k, dx, me_c)
        return remote(out.at[1, 2 * k + dx, :, y], near_in.at[k - relayed, n], near_sem, (k - relayed) * 4 + n, at(y, d))

    def direct(k):
        return range(3 if k == last else 4)

    def do_b(k):
        c_copy(k).wait_recv()
        out[1, 2 * k + 1, second, me_g] = out[1, 2 * k + 1, second, me_g] + c_in[k]
        b_copy(k).start()

    def do_e(k):
        a_copy(k).wait_recv()
        out[1, 2 * k, first, y_g] = out[1, 2 * k, first, y_g] + a_in[k, :, y_g]
        e_copy(k).start()

    def do_f(k):
        b_copy(k).wait_recv()
        d_copy(k).wait_recv()
        f_out[k, second] = out[1, 2 * k, second, me_g] + b_in[k] + d_in[k]
        e_copy(k).wait_recv()
        f_out[k, first] = out[1, 2 * k, first, me_g] + a_in[k, :, me_g] + e_in[k]
        f_copy(k).start()

    steps = [(k, dx) for dx in (1, 0) for k in range(relayed)]
    steps += [(last, 1), (relayed, 1), (relayed, 0), (last, 0)]
    total_steps = len(steps)

    def iteration(turn, carry):
        is_p = jnp.logical_or(turn == 0, jnp.logical_and(lax.rem(turn, 2) == 1, turn < 2 * total_steps - 1))
        step = jnp.where(is_p, lax.div(turn + 1, 2), lax.div(jnp.maximum(turn - 1, 0), 2))
        k = pick(step, [a for a, _ in steps])
        dx = pick(step, [a for _, a in steps])
        n = 2 * k + dx
        role = jnp.where(is_p, 0, 1)
        for y, q, piece in block(dev_of(k, dx, jnp.where(is_p, 1 - me_c, me_c))):
            out[role, n, q, y] = piece

        @pl.when(turn == 0)
        def _():
            pl.semaphore_wait(barrier, everyone - 1)

        @pl.when(is_p)
        def _():
            pair_copy(n).start()

            @pl.when(step >= relayed + 3)
            def _():
                @pl.when(step < 2 * relayed + 3)
                def _():
                    do_f(step - relayed - 3)

        @pl.when(jnp.logical_not(is_p))
        def _():
            pair_copy(n).wait_recv()
            out[1, n] = out[1, n] + pair_in[n]

            @pl.when(k < relayed)
            def _():
                @pl.when(dx == 1)
                def _():
                    a_copy(k).start()
                    c_copy(k).start()

                @pl.when(dx == 0)
                def _():
                    d_copy(k).start()
                    do_e(k)
                    do_b(k)

            @pl.when(k >= relayed)
            def _():
                @pl.when(dx == 1)
                def _():
                    direct_copy(k, 0).start()
                    direct_copy(k, 1).start()

                @pl.when(dx == 0)
                def _():
                    direct_copy(k, 2).start()

                    @pl.when(k < last)
                    def _():
                        direct_copy(k, 3).start()

        return carry

    lax.fori_loop(0, 2 * total_steps, iteration, 0)

    hist = out[1, 2 * last, :, me_g]
    for k in range(relayed):
        f_copy(k).wait_recv()
        hist = hist + f_in[k]
    for k in range(relayed, planes):
        for number in direct(k):
            direct_copy(k, number).wait_recv()
            hist = hist + near_in[k - relayed, number]

    usable = lax.rem(lane, width) < leaves
    keep = lax.broadcasted_iota(jnp.int32, (BINS, LANES), 0) < BINS - 1
    lane8 = lax.broadcasted_iota(jnp.int32, (8, LANES), 1)
    row8 = lax.broadcasted_iota(jnp.int32, (8, LANES), 0)
    tile = jnp.full((8, LANES), -jnp.inf, jnp.float32)
    for q in range(quads):
        left_grad = hist[q]
        left_hess = jnp.where(usable, pltpu.roll(left_grad, LANES - leaves, 1), 0.0)
        total_grad, total_hess = left_grad[BINS - 1:, :], left_hess[BINS - 1:, :]
        right_grad = total_grad - left_grad
        value = left_grad * left_grad / (left_hess + reg_lambda)
        value = value + right_grad * right_grad / (total_hess - left_hess + reg_lambda)
        value = value - total_grad * total_grad / (total_hess + reg_lambda)
        value = jnp.where(keep, value, -jnp.inf)
        best = jnp.broadcast_to(jnp.max(value, axis=0, keepdims=True), (8, LANES))
        for s in range(slots):
            moved = pltpu.roll(best, LANES - s * width, 1) if s else best
            tile = jnp.where(row8 == q * slots + s, moved, tile)
    top = jnp.max(tile, axis=0, keepdims=True)
    tile = jnp.where(row8 == 7, top, tile)
    gain_out[...] = tile

    gain_copy = remote(gain_out, gain_in, gain_sem, 0, y_dev)
    gain_copy.start()

    def best_copy(step):
        return remote(gain_out.at[pl.ds(7, 1)], best_in.at[step], best_sem, step, nth(step))

    for step in range(1, everyone):
        if step != devs:
            best_copy(step).start()
    for n in range(2 * planes):
        pair_copy(n).wait_send()
    for k in range(relayed):
        for make in (a_copy, b_copy, c_copy, d_copy, e_copy, f_copy):
            make(k).wait_send()
    for k in range(relayed, planes):
        for number in direct(k):
            direct_copy(k, number).wait_send()
    gain_copy.wait()
    other = gain_in[...]
    top = jnp.maximum(top, other[7:8, :])
    low_tile = jnp.where(me_g == 0, tile, other)
    high_tile = jnp.where(me_g == 0, other, tile)
    gain = jnp.where(row8 < own_features, low_tile, pltpu.roll(high_tile, own_features, 0))
    done_ref[0] = jnp.where(me_g == 0, gain, pltpu.roll(gain, LANES - own_leaves, 1))
    for step in range(1, everyone):
        if step != devs:
            best_copy(step).wait()
            top = jnp.maximum(top, best_in[step])
    top = jnp.broadcast_to(top, (8, LANES))
    done_ref[1] = jnp.where(me_g == 0, top, pltpu.roll(top, LANES - own_leaves, 1))


def finish(done_ref, gain_ref, best_ref):
    gain_ref[...] = done_ref[0, :gain_ref.shape[0], :gain_ref.shape[1]]
    best_ref[...] = done_ref[1, 0, :best_ref.shape[0]]


def kernel_body(groups, devs, bin_index, gradient, hessian, child_id, smaller_side):
    rows, features = bin_index.shape
    leaves = smaller_side.shape[0]
    per_dev = features // devs
    own_features = per_dev // groups
    own_leaves = leaves // groups
    slots = LANES // (2 * leaves)
    quads = own_features // slots
    half = quads // 2
    planes = devs // 4
    relayed = planes - 2
    everyone = groups * devs
    vmem = pl.BlockSpec(memory_space=pltpu.VMEM)
    hbm = pl.BlockSpec(memory_space=pltpu.HBM)

    def floats(*shape):
        return pltpu.VMEM(shape + (BINS, LANES), jnp.float32)

    def sems(number):
        return pltpu.SemaphoreType.DMA((2, number))

    done = pl.pallas_call(
        functools.partial(kernel, groups, devs, leaves),
        out_shape=jax.ShapeDtypeStruct((2, 8, LANES), jnp.float32),
        in_specs=[hbm] * 5,
        out_specs=vmem,
        scratch_shapes=[
            pltpu.VMEM((rows, features), jnp.int32),
            pltpu.VMEM((1, leaves), jnp.int32),
            pltpu.VMEM((rows // LANES, LANES), jnp.bfloat16),
            pltpu.VMEM((rows // LANES, LANES), jnp.bfloat16),
            pltpu.VMEM((rows // LANES, LANES), jnp.int32),
            pltpu.VMEM((3, rows // LANES, LANES), jnp.float32),
            pltpu.SemaphoreType.DMA((rows // STEP_ROWS,)),
            pltpu.SemaphoreType.DMA((4,)),
            pltpu.VMEM((features, rows), jnp.float32),
            pltpu.VMEM((LANES, rows), jnp.bfloat16),
            floats(2, 2 * planes, quads, groups),
            floats(2 * planes, quads, groups),
            floats(relayed, half, groups),
            floats(relayed, half),
            floats(relayed, half),
            floats(relayed, half),
            floats(relayed, half),
            floats(relayed, quads),
            floats(relayed, quads),
            floats(2, 4, quads),
            pltpu.VMEM((8, LANES), jnp.float32),
            pltpu.VMEM((8, LANES), jnp.float32),
            pltpu.VMEM((everyone, 1, LANES), jnp.float32),
            sems(2 * planes),
            sems(relayed),
            sems(relayed),
            sems(relayed),
            sems(relayed),
            sems(relayed),
            sems(relayed),
            sems(8),
            sems(1),
            sems(everyone),
        ],
        compiler_params=pltpu.CompilerParams(
            collective_id=0, has_side_effects=True, vmem_limit_bytes=63 * 1024 * 1024
        ),
    )(
        bin_index, gradient.reshape(rows // LANES, LANES), hessian.reshape(rows // LANES, LANES),
        child_id.reshape(rows // LANES, LANES), smaller_side.reshape(1, leaves),
    )
    gain, best = pl.pallas_call(
        finish,
        out_shape=(
            jax.ShapeDtypeStruct((per_dev, own_leaves), jnp.float32),
            jax.ShapeDtypeStruct((own_leaves,), jnp.float32),
        ),
        in_specs=[vmem],
        out_specs=(vmem, vmem),
    )(done)
    return (gain.T, best)


def fits(groups, devs, leaves, features, rows):
    planes = devs // 4
    if groups != 2 or devs % 4 or planes != 4 or leaves != 32:
        return False
    return features == 8 * devs and rows % KCHUNK == 0


def solution(mesh):
    in_specs = (
        P(("group", "dev"), None),
        P(("group", "dev")),
        P(("group", "dev")),
        P(("group", "dev")),
        P(),
    )
    out_specs = (P("group", "dev"), P("group"))
    groups, devs = mesh.shape["group"], mesh.shape["dev"]

    def body(bin_index, gradient, hessian, child_id, smaller_side):
        rows, features = bin_index.shape
        args = (bin_index, gradient, hessian, child_id, smaller_side)
        if fits(groups, devs, smaller_side.shape[0], features, rows):
            return kernel_body(groups, devs, *args)
        return plain_body(*args)

    return jax.shard_map(body, mesh=mesh, in_specs=in_specs, out_specs=out_specs, check_vma=False)
```

```python
import functools

import jax
import jax.numpy as jnp
from jax import lax
from jax.experimental import pallas as pl
from jax.experimental.pallas import tpu as pltpu
from jax.sharding import PartitionSpec as P

BINS = 64
LANES = 128
KCHUNK = 1024
STEP_ROWS = 1024


reg_lambda = 1.0


def split_gains(hist_grad, hist_hess):
    left_grad = jnp.cumsum(hist_grad, axis=-1)[..., :-1]
    left_hess = jnp.cumsum(hist_hess, axis=-1)[..., :-1]
    total_grad = jnp.sum(hist_grad, axis=-1, keepdims=True)
    total_hess = jnp.sum(hist_hess, axis=-1, keepdims=True)
    right_grad = total_grad - left_grad
    value = left_grad * left_grad / (left_hess + reg_lambda)
    value = value + right_grad * right_grad / (total_hess - left_hess + reg_lambda)
    value = value - total_grad * total_grad / (total_hess + reg_lambda)
    return jnp.max(value, axis=-1)


def plain_body(bin_index, gradient, hessian, child_id, smaller_side):
    leaves = smaller_side.shape[0]
    features = bin_index.shape[1]
    target = 2 * jnp.arange(leaves, dtype=jnp.int32)[None, :] + smaller_side[None, :]
    chosen = child_id[:, None] == target
    nothing = jnp.zeros((), jnp.bfloat16)
    weights = jnp.concatenate(
        [
            jnp.where(chosen, gradient[:, None], nothing),
            jnp.where(chosen, hessian[:, None], nothing),
        ],
        axis=1,
    )
    levels = jnp.arange(BINS, dtype=jnp.int32)

    def one_feature(column):
        onehot = (column[:, None] == levels[None, :]).astype(jnp.bfloat16)
        product = lax.dot_general(
            weights, onehot, (((0,), (0,)), ((), ())), preferred_element_type=jnp.float32
        )
        return product.reshape(2, leaves, BINS).transpose(1, 0, 2).reshape(leaves, 2 * BINS)

    stacked = lax.map(one_feature, bin_index.T)
    owned = lax.psum_scatter(stacked, "dev", scatter_dimension=0, tiled=True)
    owned = lax.psum_scatter(owned, "group", scatter_dimension=1, tiled=True)
    hist_grad = owned[:, :, :BINS].transpose(1, 0, 2)
    hist_hess = owned[:, :, BINS:].transpose(1, 0, 2)
    best_gain = split_gains(hist_grad, hist_hess)
    child_best = lax.pmax(jnp.max(best_gain, axis=1), "dev")
    return (best_gain, child_best)


def kernel(
    groups, devs, leaves,
    bins_ref, grad_ref, hess_ref, child_ref, side_ref,
    done_ref,
    bins_v, side_v, grad_v, hess_v, child_v, values, bins_sem, small_sem,
    bins_t, weights, out, pair_in, a_in, b_in, c_in, d_in, e_in, f_out, f_in, near_in,
    gain_out, gain_in, best_in,
    pair_sem, a_sem, b_sem, c_sem, d_sem, e_sem, f_sem, near_sem, gain_sem, best_sem,
):
    rows, features = bins_ref.shape
    per_dev = features // devs
    own_features = per_dev // groups
    own_leaves = leaves // groups
    width = 2 * leaves
    slots = LANES // width
    quads = own_features // slots
    half = quads // 2
    planes = devs // 4
    last = planes - 1
    relayed = last - 1
    me_g = lax.axis_index("group")
    me_d = lax.axis_index("dev")
    me_c = lax.rem(me_d, 2)
    me_j = lax.div(me_d, 2)
    me_x = lax.rem(me_j, 2)
    me_z = lax.div(me_j, 2)
    barrier = pltpu.get_barrier_semaphore()
    step_rows = STEP_ROWS
    everyone = groups * devs

    def bins_copy(number):
        here = pl.ds(pl.multiple_of(number * step_rows, step_rows), step_rows)
        return pltpu.make_async_copy(bins_ref.at[here, :], bins_v.at[here, :], bins_sem.at[number])

    small = [
        pltpu.make_async_copy(source, place, small_sem.at[number])
        for number, (source, place) in enumerate(
            [(side_ref, side_v), (child_ref, child_v), (grad_ref, grad_v), (hess_ref, hess_v)]
        )
    ]
    for copy in small:
        copy.start()

    def start_bins(number, carry):
        bins_copy(number).start()
        return carry

    lax.fori_loop(0, rows // step_rows, start_bins, 0)

    def at(g, d):
        return {"group": g, "dev": d}

    def nth(step):
        other = lax.rem(me_g * devs + me_d + step, everyone)
        return at(lax.div(other, devs), lax.rem(other, devs))

    def greet(step, carry):
        pl.semaphore_signal(barrier, inc=1, device_id=nth(step), device_id_type=pl.DeviceIdType.MESH)
        return carry

    lax.fori_loop(1, everyone, greet, 0)

    pair_row = lax.broadcasted_iota(jnp.int32, (leaves, leaves), 0)
    pair_lane = lax.broadcasted_iota(jnp.int32, (leaves, leaves), 1)

    for copy in small:
        copy.wait()

    side = jnp.where(pair_lane == pair_row, side_v[...].astype(jnp.float32), 0.0)
    target = jnp.sum(side, axis=1, keepdims=True) + 2.0 * pair_row[:, :1].astype(jnp.float32)
    target = jnp.broadcast_to(target, (leaves, LANES)).astype(jnp.bfloat16)
    values[0] = grad_v[...].astype(jnp.float32)
    values[1] = hess_v[...].astype(jnp.float32)
    values[2] = child_v[...].astype(jnp.float32)
    no_weight = jnp.zeros((), jnp.bfloat16)

    def prepare(number, carry):
        here = pl.ds(pl.multiple_of(number * step_rows, step_rows), step_rows)
        for piece in range(step_rows // LANES):
            row = number * (step_rows // LANES) + piece
            there = pl.ds(pl.multiple_of(row * LANES, LANES), LANES)

            def spread(kind):
                return jnp.broadcast_to(values[kind, pl.ds(row, 1), :], (leaves, LANES)).astype(jnp.bfloat16)

            chosen = spread(2) == target
            for kind in range(2):
                value = jnp.where(chosen, spread(kind), no_weight)
                for s in range(slots):
                    start = s * width + kind * leaves
                    weights[start:start + leaves, there] = value
        bins_copy(number).wait()
        bins_t[:, here] = bins_v[here, :].astype(jnp.float32).T
        return carry

    lax.fori_loop(0, rows // step_rows, prepare, 0)

    chunk = min(rows, KCHUNK)
    pack = 16
    level = lax.broadcasted_iota(jnp.int32, (pack, chunk), 0).astype(jnp.float32).astype(jnp.bfloat16)
    one = jnp.ones((), jnp.bfloat16)
    zero = jnp.zeros((), jnp.bfloat16)
    lane = lax.broadcasted_iota(jnp.int32, (BINS, LANES), 1)

    def block(d):
        base = pl.multiple_of(d * per_dev, per_dev)
        total = None
        for start in range(0, rows, chunk):
            parts = []
            levels = bins_t[pl.ds(base, per_dev), start:start + chunk]
            for f in range(per_dev):
                row = jnp.broadcast_to(levels[f:f + 1, :], (pack, chunk)).astype(jnp.bfloat16)
                for low in range(0, BINS, pack):
                    parts.append(jnp.where(row <= level + jnp.bfloat16(low), one, zero))
            below = jnp.concatenate(parts, axis=0)
            product = lax.dot_general(
                below, weights[:, start:start + chunk], (((1,), (1,)), ((), ())),
                preferred_element_type=jnp.float32,
            )
            total = product if total is None else total + product
        result = []
        for y in range(groups):
            for q in range(quads):
                piece = None
                for s in range(slots):
                    f = (y * quads + q) * slots + s
                    here = total[f * BINS:(f + 1) * BINS, :]
                    piece = here if piece is None else jnp.where(lane >= s * width, here, piece)
                result.append((y, q, piece))
        return result

    def remote(source, place, sem, index, device):
        return pltpu.make_async_remote_copy(
            src_ref=source, dst_ref=place, send_sem=sem.at[0, index], recv_sem=sem.at[1, index],
            device_id=device, device_id_type=pl.DeviceIdType.MESH,
        )

    def pick(index, choices):
        result = choices[-1]
        for number in range(len(choices) - 1):
            result = jnp.where(index == number, choices[number], result)
        return result

    def flipped(turn):
        result, bit = 0, 1
        while bit < planes:
            digit = lax.rem(lax.div(me_z, bit), 2)
            result = result + bit * (1 - digit if (turn // bit) % 2 else digit)
            bit *= 2
        return result

    planes_of = [flipped(last - k) for k in range(planes)]

    def plane(k):
        return planes_of[k] if isinstance(k, int) else pick(k, planes_of)

    def dev_of(k, dx, core):
        x = jnp.where(dx == 1, 1 - me_x, me_x)
        return (plane(k) * 2 + x) * 2 + core

    pair_dev = at(me_g, me_j * 2 + 1 - me_c)
    x_dev_d = (me_z * 2 + 1 - me_x) * 2 + me_c
    x_dev = at(me_g, x_dev_d)
    y_g = 1 - me_g
    y_dev = at(y_g, me_d)
    diag_dev = at(y_g, x_dev_d)

    def pair_copy(n):
        return remote(out.at[0, n], pair_in.at[n], pair_sem, n, pair_dev)

    first = slice(0, half)
    second = slice(half, quads)

    def a_copy(k):
        return remote(out.at[1, 2 * k + 1, first], a_in.at[k], a_sem, k, x_dev)

    def b_copy(k):
        return remote(out.at[1, 2 * k + 1, second, me_g], b_in.at[k], b_sem, k, x_dev)

    def c_copy(k):
        return remote(out.at[1, 2 * k + 1, second, y_g], c_in.at[k], c_sem, k, y_dev)

    def d_copy(k):
        return remote(out.at[1, 2 * k, second, y_g], d_in.at[k], d_sem, k, y_dev)

    def e_copy(k):
        return remote(out.at[1, 2 * k, first, y_g], e_in.at[k], e_sem, k, y_dev)

    def f_copy(k):
        d = (plane(k) * 2 + me_x) * 2 + me_c
        return remote(f_out.at[k], f_in.at[k], f_sem, k, at(me_g, d))

    def direct_copy(k, n):
        dx, y = ((1, y_g), (1, me_g), (0, y_g), (0, me_g))[n]
        d = dev_of(k, dx, me_c)
        return remote(out.at[1, 2 * k + dx, :, y], near_in.at[k - relayed, n], near_sem, (k - relayed) * 4 + n, at(y, d))

    def direct(k):
        return range(3 if k == last else 4)

    def do_b(k):
        c_copy(k).wait_recv()
        out[1, 2 * k + 1, second, me_g] = out[1, 2 * k + 1, second, me_g] + c_in[k]
        b_copy(k).start()

    def do_e(k):
        a_copy(k).wait_recv()
        out[1, 2 * k, first, y_g] = out[1, 2 * k, first, y_g] + a_in[k, :, y_g]
        e_copy(k).start()

    def do_f(k):
        b_copy(k).wait_recv()
        d_copy(k).wait_recv()
        f_out[k, second] = out[1, 2 * k, second, me_g] + b_in[k] + d_in[k]
        e_copy(k).wait_recv()
        f_out[k, first] = out[1, 2 * k, first, me_g] + a_in[k, :, me_g] + e_in[k]
        f_copy(k).start()

    steps = [(k, dx) for dx in (1, 0) for k in range(relayed)]
    steps += [(relayed, 1), (last, 1), (relayed, 0), (last, 0)]
    total_steps = len(steps)

    def group_of(step):
        k = pick(step, [a for a, _ in steps])
        dx = pick(step, [a for _, a in steps])
        return k, dx, 2 * k + dx

    def work(step, is_p):
        k, dx, n = group_of(step)
        role = jnp.where(is_p, 0, 1)
        for y, q, piece in block(dev_of(k, dx, jnp.where(is_p, 1 - me_c, me_c))):
            out[role, n, q, y] = piece

    def send_pair(step):
        pair_copy(group_of(step)[2]).start()

    def pass_on(step, carry):
        k, dx, n = group_of(step)
        pair_copy(n).wait_recv()
        out[1, n] = out[1, n] + pair_in[n]

        @pl.when(k < relayed)
        def _():
            @pl.when(dx == 1)
            def _():
                a_copy(k).start()
                c_copy(k).start()

            @pl.when(dx == 0)
            def _():
                d_copy(k).start()
                do_e(k)
                do_b(k)

        @pl.when(k >= relayed)
        def _():
            @pl.when(dx == 1)
            def _():
                direct_copy(k, 0).start()
                direct_copy(k, 1).start()

            @pl.when(dx == 0)
            def _():
                direct_copy(k, 2).start()

                @pl.when(k < last)
                def _():
                    direct_copy(k, 3).start()

        return carry

    def iteration(turn, carry):
        work(jnp.maximum(turn - 1, 0), turn == 0)
        work(jnp.minimum(turn + 1, total_steps - 1), turn < total_steps - 1)

        @pl.when(turn == 0)
        def _():
            pl.semaphore_wait(barrier, everyone - 1)
            send_pair(0)

        @pl.when(turn < total_steps - 1)
        def _():
            send_pair(turn + 1)

        lax.fori_loop(
            jnp.maximum(turn - 1, 0), jnp.where(turn == total_steps - 1, total_steps, turn), pass_on, 0
        )

        @pl.when(turn >= 2 * relayed + 1)
        def _():
            @pl.when(turn < 2 * relayed + 1 + relayed)
            def _():
                do_f(turn - (2 * relayed + 1))

        return carry

    lax.fori_loop(0, total_steps, iteration, 0)

    hist = out[1, 2 * last, :, me_g]
    for k in range(relayed):
        f_copy(k).wait_recv()
        hist = hist + f_in[k]
    for k in range(relayed, planes):
        for number in direct(k):
            direct_copy(k, number).wait_recv()
            hist = hist + near_in[k - relayed, number]

    usable = lax.rem(lane, width) < leaves
    keep = lax.broadcasted_iota(jnp.int32, (BINS, LANES), 0) < BINS - 1
    lane8 = lax.broadcasted_iota(jnp.int32, (8, LANES), 1)
    row8 = lax.broadcasted_iota(jnp.int32, (8, LANES), 0)
    tile = jnp.full((8, LANES), -jnp.inf, jnp.float32)
    for q in range(quads):
        left_grad = hist[q]
        left_hess = jnp.where(usable, pltpu.roll(left_grad, LANES - leaves, 1), 0.0)
        total_grad, total_hess = left_grad[BINS - 1:, :], left_hess[BINS - 1:, :]
        right_grad = total_grad - left_grad
        value = left_grad * left_grad / (left_hess + reg_lambda)
        value = value + right_grad * right_grad / (total_hess - left_hess + reg_lambda)
        value = value - total_grad * total_grad / (total_hess + reg_lambda)
        value = jnp.where(keep, value, -jnp.inf)
        best = jnp.broadcast_to(jnp.max(value, axis=0, keepdims=True), (8, LANES))
        for s in range(slots):
            moved = pltpu.roll(best, LANES - s * width, 1) if s else best
            tile = jnp.where(row8 == q * slots + s, moved, tile)
    top = jnp.max(tile, axis=0, keepdims=True)
    tile = jnp.where(row8 == 7, top, tile)
    gain_out[...] = tile

    gain_copy = remote(gain_out, gain_in, gain_sem, 0, y_dev)
    gain_copy.start()

    def best_copy(step):
        return remote(gain_out.at[pl.ds(7, 1)], best_in.at[step], best_sem, step, nth(step))

    for step in range(1, everyone):
        if step != devs:
            best_copy(step).start()
    for n in range(2 * planes):
        pair_copy(n).wait_send()
    for k in range(relayed):
        for make in (a_copy, b_copy, c_copy, d_copy, e_copy, f_copy):
            make(k).wait_send()
    for k in range(relayed, planes):
        for number in direct(k):
            direct_copy(k, number).wait_send()
    gain_copy.wait()
    other = gain_in[...]
    top = jnp.maximum(top, other[7:8, :])
    low_tile = jnp.where(me_g == 0, tile, other)
    high_tile = jnp.where(me_g == 0, other, tile)
    gain = jnp.where(row8 < own_features, low_tile, pltpu.roll(high_tile, own_features, 0))
    done_ref[0] = jnp.where(me_g == 0, gain, pltpu.roll(gain, LANES - own_leaves, 1))
    for step in range(1, everyone):
        if step != devs:
            best_copy(step).wait()
            top = jnp.maximum(top, best_in[step])
    top = jnp.broadcast_to(top, (8, LANES))
    done_ref[1] = jnp.where(me_g == 0, top, pltpu.roll(top, LANES - own_leaves, 1))


def finish(done_ref, gain_ref, best_ref):
    gain_ref[...] = done_ref[0, :gain_ref.shape[0], :gain_ref.shape[1]]
    best_ref[...] = done_ref[1, 0, :best_ref.shape[0]]


def kernel_body(groups, devs, bin_index, gradient, hessian, child_id, smaller_side):
    rows, features = bin_index.shape
    leaves = smaller_side.shape[0]
    per_dev = features // devs
    own_features = per_dev // groups
    own_leaves = leaves // groups
    slots = LANES // (2 * leaves)
    quads = own_features // slots
    half = quads // 2
    planes = devs // 4
    relayed = planes - 2
    everyone = groups * devs
    vmem = pl.BlockSpec(memory_space=pltpu.VMEM)
    hbm = pl.BlockSpec(memory_space=pltpu.HBM)

    def floats(*shape):
        return pltpu.VMEM(shape + (BINS, LANES), jnp.float32)

    def sems(number):
        return pltpu.SemaphoreType.DMA((2, number))

    done = pl.pallas_call(
        functools.partial(kernel, groups, devs, leaves),
        out_shape=jax.ShapeDtypeStruct((2, 8, LANES), jnp.float32),
        in_specs=[hbm] * 5,
        out_specs=vmem,
        scratch_shapes=[
            pltpu.VMEM((rows, features), jnp.int32),
            pltpu.VMEM((1, leaves), jnp.int32),
            pltpu.VMEM((rows // LANES, LANES), jnp.bfloat16),
            pltpu.VMEM((rows // LANES, LANES), jnp.bfloat16),
            pltpu.VMEM((rows // LANES, LANES), jnp.int32),
            pltpu.VMEM((3, rows // LANES, LANES), jnp.float32),
            pltpu.SemaphoreType.DMA((rows // STEP_ROWS,)),
            pltpu.SemaphoreType.DMA((4,)),
            pltpu.VMEM((features, rows), jnp.float32),
            pltpu.VMEM((LANES, rows), jnp.bfloat16),
            floats(2, 2 * planes, quads, groups),
            floats(2 * planes, quads, groups),
            floats(relayed, half, groups),
            floats(relayed, half),
            floats(relayed, half),
            floats(relayed, half),
            floats(relayed, half),
            floats(relayed, quads),
            floats(relayed, quads),
            floats(2, 4, quads),
            pltpu.VMEM((8, LANES), jnp.float32),
            pltpu.VMEM((8, LANES), jnp.float32),
            pltpu.VMEM((everyone, 1, LANES), jnp.float32),
            sems(2 * planes),
            sems(relayed),
            sems(relayed),
            sems(relayed),
            sems(relayed),
            sems(relayed),
            sems(relayed),
            sems(8),
            sems(1),
            sems(everyone),
        ],
        compiler_params=pltpu.CompilerParams(
            collective_id=0, has_side_effects=True, vmem_limit_bytes=63 * 1024 * 1024
        ),
    )(
        bin_index, gradient.reshape(rows // LANES, LANES), hessian.reshape(rows // LANES, LANES),
        child_id.reshape(rows // LANES, LANES), smaller_side.reshape(1, leaves),
    )
    gain, best = pl.pallas_call(
        finish,
        out_shape=(
            jax.ShapeDtypeStruct((per_dev, own_leaves), jnp.float32),
            jax.ShapeDtypeStruct((own_leaves,), jnp.float32),
        ),
        in_specs=[vmem],
        out_specs=(vmem, vmem),
    )(done)
    return (gain.T, best)


def fits(groups, devs, leaves, features, rows):
    planes = devs // 4
    if groups != 2 or devs % 4 or planes != 4 or leaves != 32:
        return False
    return features == 8 * devs and rows % KCHUNK == 0


def solution(mesh):
    in_specs = (
        P(("group", "dev"), None),
        P(("group", "dev")),
        P(("group", "dev")),
        P(("group", "dev")),
        P(),
    )
    out_specs = (P("group", "dev"), P("group"))
    groups, devs = mesh.shape["group"], mesh.shape["dev"]

    def body(bin_index, gradient, hessian, child_id, smaller_side):
        rows, features = bin_index.shape
        args = (bin_index, gradient, hessian, child_id, smaller_side)
        if fits(groups, devs, smaller_side.shape[0], features, rows):
            return kernel_body(groups, devs, *args)
        return plain_body(*args)

    return jax.shard_map(body, mesh=mesh, in_specs=in_specs, out_specs=out_specs, check_vma=False)
```

```python
import functools

import jax
import jax.numpy as jnp
from jax import lax
from jax.experimental import pallas as pl
from jax.experimental.pallas import tpu as pltpu
from jax.sharding import PartitionSpec as P

BINS = 64
LANES = 128
KCHUNK = 1024
STEP_ROWS = 1024


reg_lambda = 1.0


def split_gains(hist_grad, hist_hess):
    left_grad = jnp.cumsum(hist_grad, axis=-1)[..., :-1]
    left_hess = jnp.cumsum(hist_hess, axis=-1)[..., :-1]
    total_grad = jnp.sum(hist_grad, axis=-1, keepdims=True)
    total_hess = jnp.sum(hist_hess, axis=-1, keepdims=True)
    right_grad = total_grad - left_grad
    value = left_grad * left_grad / (left_hess + reg_lambda)
    value = value + right_grad * right_grad / (total_hess - left_hess + reg_lambda)
    value = value - total_grad * total_grad / (total_hess + reg_lambda)
    return jnp.max(value, axis=-1)


def plain_body(bin_index, gradient, hessian, child_id, smaller_side):
    leaves = smaller_side.shape[0]
    features = bin_index.shape[1]
    target = 2 * jnp.arange(leaves, dtype=jnp.int32)[None, :] + smaller_side[None, :]
    chosen = child_id[:, None] == target
    nothing = jnp.zeros((), jnp.bfloat16)
    weights = jnp.concatenate(
        [
            jnp.where(chosen, gradient[:, None], nothing),
            jnp.where(chosen, hessian[:, None], nothing),
        ],
        axis=1,
    )
    levels = jnp.arange(BINS, dtype=jnp.int32)

    def one_feature(column):
        onehot = (column[:, None] == levels[None, :]).astype(jnp.bfloat16)
        product = lax.dot_general(
            weights, onehot, (((0,), (0,)), ((), ())), preferred_element_type=jnp.float32
        )
        return product.reshape(2, leaves, BINS).transpose(1, 0, 2).reshape(leaves, 2 * BINS)

    stacked = lax.map(one_feature, bin_index.T)
    owned = lax.psum_scatter(stacked, "dev", scatter_dimension=0, tiled=True)
    owned = lax.psum_scatter(owned, "group", scatter_dimension=1, tiled=True)
    hist_grad = owned[:, :, :BINS].transpose(1, 0, 2)
    hist_hess = owned[:, :, BINS:].transpose(1, 0, 2)
    best_gain = split_gains(hist_grad, hist_hess)
    child_best = lax.pmax(jnp.max(best_gain, axis=1), "dev")
    return (best_gain, child_best)


def kernel(
    groups, devs, leaves,
    bins_ref, grad_ref, hess_ref, child_ref, side_ref,
    done_ref,
    bins_v, side_v, grad_v, hess_v, child_v, values, bins_sem, small_sem,
    bins_t, weights, out, pair_in, a_in, b_in, c_in, d_in, e_in, f_out, f_in, near_in,
    gain_out, gain_in, best_in,
    pair_sem, a_sem, b_sem, c_sem, d_sem, e_sem, f_sem, near_sem, gain_sem, best_sem,
):
    rows, features = bins_ref.shape
    per_dev = features // devs
    own_features = per_dev // groups
    own_leaves = leaves // groups
    width = 2 * leaves
    slots = LANES // width
    quads = own_features // slots
    half = quads // 2
    planes = devs // 4
    last = planes - 1
    relayed = last - 1
    me_g = lax.axis_index("group")
    me_d = lax.axis_index("dev")
    me_c = lax.rem(me_d, 2)
    me_j = lax.div(me_d, 2)
    me_x = lax.rem(me_j, 2)
    me_z = lax.div(me_j, 2)
    barrier = pltpu.get_barrier_semaphore()
    step_rows = STEP_ROWS
    everyone = groups * devs

    def bins_copy(number):
        here = pl.ds(pl.multiple_of(number * step_rows, step_rows), step_rows)
        return pltpu.make_async_copy(bins_ref.at[here, :], bins_v.at[here, :], bins_sem.at[number])

    small = [
        pltpu.make_async_copy(source, place, small_sem.at[number])
        for number, (source, place) in enumerate(
            [(side_ref, side_v), (child_ref, child_v), (grad_ref, grad_v), (hess_ref, hess_v)]
        )
    ]
    for copy in small:
        copy.start()

    def start_bins(number, carry):
        bins_copy(number).start()
        return carry

    lax.fori_loop(0, rows // step_rows, start_bins, 0)

    def at(g, d):
        return {"group": g, "dev": d}

    def nth(step):
        other = lax.rem(me_g * devs + me_d + step, everyone)
        return at(lax.div(other, devs), lax.rem(other, devs))

    def greet(step, carry):
        pl.semaphore_signal(barrier, inc=1, device_id=nth(step), device_id_type=pl.DeviceIdType.MESH)
        return carry

    lax.fori_loop(1, everyone, greet, 0)

    pair_row = lax.broadcasted_iota(jnp.int32, (leaves, leaves), 0)
    pair_lane = lax.broadcasted_iota(jnp.int32, (leaves, leaves), 1)

    for copy in small:
        copy.wait()

    side = jnp.where(pair_lane == pair_row, side_v[...].astype(jnp.float32), 0.0)
    target = jnp.sum(side, axis=1, keepdims=True) + 2.0 * pair_row[:, :1].astype(jnp.float32)
    target = jnp.broadcast_to(target, (leaves, LANES)).astype(jnp.bfloat16)
    values[0] = grad_v[...].astype(jnp.float32)
    values[1] = hess_v[...].astype(jnp.float32)
    values[2] = child_v[...].astype(jnp.float32)
    no_weight = jnp.zeros((), jnp.bfloat16)

    def prepare(number, carry):
        here = pl.ds(pl.multiple_of(number * step_rows, step_rows), step_rows)
        for piece in range(step_rows // LANES):
            row = number * (step_rows // LANES) + piece
            there = pl.ds(pl.multiple_of(row * LANES, LANES), LANES)

            def spread(kind):
                return jnp.broadcast_to(values[kind, pl.ds(row, 1), :], (leaves, LANES)).astype(jnp.bfloat16)

            chosen = spread(2) == target
            for kind in range(2):
                value = jnp.where(chosen, spread(kind), no_weight)
                for s in range(slots):
                    start = s * width + kind * leaves
                    weights[start:start + leaves, there] = value
        return carry

    def turn_bins(number, carry):
        here = pl.ds(pl.multiple_of(number * step_rows, step_rows), step_rows)
        bins_copy(number).wait()
        bins_t[:, here] = bins_v[here, :].astype(jnp.float32).astype(jnp.bfloat16).T.astype(jnp.float32)
        return carry

    lax.fori_loop(0, rows // step_rows, prepare, 0)
    lax.fori_loop(0, rows // step_rows, turn_bins, 0)

    chunk = min(rows, KCHUNK)
    pack = 16
    level = lax.broadcasted_iota(jnp.int32, (pack, chunk), 0).astype(jnp.float32).astype(jnp.bfloat16)
    one = jnp.ones((), jnp.bfloat16)
    zero = jnp.zeros((), jnp.bfloat16)
    lane = lax.broadcasted_iota(jnp.int32, (BINS, LANES), 1)

    def block(d):
        base = pl.multiple_of(d * per_dev, per_dev)
        total = None
        for start in range(0, rows, chunk):
            parts = []
            levels = bins_t[pl.ds(base, per_dev), start:start + chunk]
            for f in range(per_dev):
                row = jnp.broadcast_to(levels[f:f + 1, :], (pack, chunk)).astype(jnp.bfloat16)
                for low in range(0, BINS, pack):
                    parts.append(jnp.where(row <= level + jnp.bfloat16(low), one, zero))
            below = jnp.concatenate(parts, axis=0)
            product = lax.dot_general(
                below, weights[:, start:start + chunk], (((1,), (1,)), ((), ())),
                preferred_element_type=jnp.float32,
            )
            total = product if total is None else total + product
        result = []
        for y in range(groups):
            for q in range(quads):
                piece = None
                for s in range(slots):
                    f = (y * quads + q) * slots + s
                    here = total[f * BINS:(f + 1) * BINS, :]
                    piece = here if piece is None else jnp.where(lane >= s * width, here, piece)
                result.append((y, q, piece))
        return result

    def remote(source, place, sem, index, device):
        return pltpu.make_async_remote_copy(
            src_ref=source, dst_ref=place, send_sem=sem.at[0, index], recv_sem=sem.at[1, index],
            device_id=device, device_id_type=pl.DeviceIdType.MESH,
        )

    def pick(index, choices):
        result = choices[-1]
        for number in range(len(choices) - 1):
            result = jnp.where(index == number, choices[number], result)
        return result

    def flipped(turn):
        result, bit = 0, 1
        while bit < planes:
            digit = lax.rem(lax.div(me_z, bit), 2)
            result = result + bit * (1 - digit if (turn // bit) % 2 else digit)
            bit *= 2
        return result

    planes_of = [flipped(last - k) for k in range(planes)]

    def plane(k):
        return planes_of[k] if isinstance(k, int) else pick(k, planes_of)

    def dev_of(k, dx, core):
        x = jnp.where(dx == 1, 1 - me_x, me_x)
        return (plane(k) * 2 + x) * 2 + core

    pair_dev = at(me_g, me_j * 2 + 1 - me_c)
    x_dev_d = (me_z * 2 + 1 - me_x) * 2 + me_c
    x_dev = at(me_g, x_dev_d)
    y_g = 1 - me_g
    y_dev = at(y_g, me_d)
    diag_dev = at(y_g, x_dev_d)

    def pair_copy(n):
        return remote(out.at[0, n], pair_in.at[n], pair_sem, n, pair_dev)

    first = slice(0, half)
    second = slice(half, quads)

    def a_copy(k):
        return remote(out.at[1, 2 * k + 1, first], a_in.at[k], a_sem, k, x_dev)

    def b_copy(k):
        return remote(out.at[1, 2 * k + 1, second, me_g], b_in.at[k], b_sem, k, x_dev)

    def c_copy(k):
        return remote(out.at[1, 2 * k + 1, second, y_g], c_in.at[k], c_sem, k, y_dev)

    def d_copy(k):
        return remote(out.at[1, 2 * k, second, y_g], d_in.at[k], d_sem, k, y_dev)

    def e_copy(k):
        return remote(out.at[1, 2 * k, first, y_g], e_in.at[k], e_sem, k, y_dev)

    def f_copy(k):
        d = (plane(k) * 2 + me_x) * 2 + me_c
        return remote(f_out.at[k], f_in.at[k], f_sem, k, at(me_g, d))

    def direct_copy(k, n):
        dx, y = ((1, y_g), (1, me_g), (0, y_g), (0, me_g))[n]
        d = dev_of(k, dx, me_c)
        return remote(out.at[1, 2 * k + dx, :, y], near_in.at[k - relayed, n], near_sem, (k - relayed) * 4 + n, at(y, d))

    def direct(k):
        return range(3 if k == last else 4)

    def do_b(k):
        c_copy(k).wait_recv()
        out[1, 2 * k + 1, second, me_g] = out[1, 2 * k + 1, second, me_g] + c_in[k]
        b_copy(k).start()

    def do_e(k):
        a_copy(k).wait_recv()
        out[1, 2 * k, first, y_g] = out[1, 2 * k, first, y_g] + a_in[k, :, y_g]
        e_copy(k).start()

    def do_f(k):
        b_copy(k).wait_recv()
        d_copy(k).wait_recv()
        f_out[k, second] = out[1, 2 * k, second, me_g] + b_in[k] + d_in[k]
        e_copy(k).wait_recv()
        f_out[k, first] = out[1, 2 * k, first, me_g] + a_in[k, :, me_g] + e_in[k]
        f_copy(k).start()

    steps = [(k, 1) for k in range(last)] + [(k, 0) for k in range(last)] + [(last, 1), (last, 0)]
    turns = len(steps)

    def group_of(step):
        k = pick(step, [a for a, _ in steps])
        dx = pick(step, [a for _, a in steps])
        return k, dx, 2 * k + dx

    def work(step, is_p):
        k, dx, n = group_of(step)
        role = jnp.where(is_p, 0, 1)
        for y, q, piece in block(dev_of(k, dx, jnp.where(is_p, 1 - me_c, me_c))):
            out[role, n, q, y] = piece

    def pass_on(step):
        k, dx, n = group_of(step)
        pair_copy(n).wait_recv()
        out[1, n] = out[1, n] + pair_in[n]

        @pl.when(k < relayed)
        def _():
            @pl.when(dx == 1)
            def _():
                a_copy(k).start()
                c_copy(k).start()

            @pl.when(dx == 0)
            def _():
                d_copy(k).start()
                do_e(k)
                do_b(k)

        @pl.when(k >= relayed)
        def _():
            @pl.when(dx == 1)
            def _():
                direct_copy(k, 0).start()
                direct_copy(k, 1).start()

            @pl.when(dx == 0)
            def _():
                direct_copy(k, 2).start()

                @pl.when(k < last)
                def _():
                    direct_copy(k, 3).start()

    def iteration(turn, carry):
        step = lax.div(turn, 2) * 2
        is_p = lax.rem(turn, 2) == 0
        work(step, is_p)
        work(step + 1, is_p)

        @pl.when(turn == 0)
        def _():
            pl.semaphore_wait(barrier, everyone - 1)

        @pl.when(is_p)
        def _():
            pair_copy(group_of(step)[2]).start()
            pair_copy(group_of(step + 1)[2]).start()

        @pl.when(jnp.logical_not(is_p))
        def _():
            for k in range(relayed - 1):
                @pl.when(turn == turns - 1 - 2 * (relayed - 1 - k))
                def _():
                    do_f(k)

            pass_on(step)
            pass_on(step + 1)

        return carry

    lax.fori_loop(0, turns - 1, iteration, 0)

    def closing(step, carry):
        work(step, False)

        pass_on(step)

        @pl.when(step == turns - 2)
        def _():
            do_f(relayed - 1)

        return carry

    lax.fori_loop(turns - 2, turns, closing, 0)

    hist = out[1, 2 * last, :, me_g]
    for k in range(relayed):
        f_copy(k).wait_recv()
        hist = hist + f_in[k]
    for k in range(relayed, planes):
        for number in direct(k):
            direct_copy(k, number).wait_recv()
            hist = hist + near_in[k - relayed, number]

    usable = lax.rem(lane, width) < leaves
    keep = lax.broadcasted_iota(jnp.int32, (BINS, LANES), 0) < BINS - 1
    lane8 = lax.broadcasted_iota(jnp.int32, (8, LANES), 1)
    row8 = lax.broadcasted_iota(jnp.int32, (8, LANES), 0)
    tile = jnp.full((8, LANES), -jnp.inf, jnp.float32)
    for q in range(quads):
        left_grad = hist[q]
        left_hess = jnp.where(usable, pltpu.roll(left_grad, LANES - leaves, 1), 0.0)
        total_grad, total_hess = left_grad[BINS - 1:, :], left_hess[BINS - 1:, :]
        right_grad = total_grad - left_grad
        value = left_grad * left_grad / (left_hess + reg_lambda)
        value = value + right_grad * right_grad / (total_hess - left_hess + reg_lambda)
        value = value - total_grad * total_grad / (total_hess + reg_lambda)
        value = jnp.where(keep, value, -jnp.inf)
        best = jnp.broadcast_to(jnp.max(value, axis=0, keepdims=True), (8, LANES))
        for s in range(slots):
            moved = pltpu.roll(best, LANES - s * width, 1) if s else best
            tile = jnp.where(row8 == q * slots + s, moved, tile)
    top = jnp.max(tile, axis=0, keepdims=True)
    tile = jnp.where(row8 == 7, top, tile)
    gain_out[...] = tile

    gain_copy = remote(gain_out, gain_in, gain_sem, 0, y_dev)
    gain_copy.start()

    def best_copy(step):
        return remote(gain_out.at[pl.ds(7, 1)], best_in.at[step], best_sem, step, nth(step))

    for step in range(1, everyone):
        if step != devs:
            best_copy(step).start()
    for n in range(2 * planes):
        pair_copy(n).wait_send()
    for k in range(relayed):
        for make in (a_copy, b_copy, c_copy, d_copy, e_copy, f_copy):
            make(k).wait_send()
    for k in range(relayed, planes):
        for number in direct(k):
            direct_copy(k, number).wait_send()
    gain_copy.wait()
    other = gain_in[...]
    top = jnp.maximum(top, other[7:8, :])
    low_tile = jnp.where(me_g == 0, tile, other)
    high_tile = jnp.where(me_g == 0, other, tile)
    gain = jnp.where(row8 < own_features, low_tile, pltpu.roll(high_tile, own_features, 0))
    done_ref[0] = jnp.where(me_g == 0, gain, pltpu.roll(gain, LANES - own_leaves, 1))
    for step in range(1, everyone):
        if step != devs:
            best_copy(step).wait()
            top = jnp.maximum(top, best_in[step])
    top = jnp.broadcast_to(top, (8, LANES))
    done_ref[1] = jnp.where(me_g == 0, top, pltpu.roll(top, LANES - own_leaves, 1))


def finish(done_ref, gain_ref, best_ref):
    gain_ref[...] = done_ref[0, :gain_ref.shape[0], :gain_ref.shape[1]]
    best_ref[...] = done_ref[1, 0, :best_ref.shape[0]]


def kernel_body(groups, devs, bin_index, gradient, hessian, child_id, smaller_side):
    rows, features = bin_index.shape
    leaves = smaller_side.shape[0]
    per_dev = features // devs
    own_features = per_dev // groups
    own_leaves = leaves // groups
    slots = LANES // (2 * leaves)
    quads = own_features // slots
    half = quads // 2
    planes = devs // 4
    relayed = planes - 2
    everyone = groups * devs
    vmem = pl.BlockSpec(memory_space=pltpu.VMEM)
    hbm = pl.BlockSpec(memory_space=pltpu.HBM)

    def floats(*shape):
        return pltpu.VMEM(shape + (BINS, LANES), jnp.float32)

    def sems(number):
        return pltpu.SemaphoreType.DMA((2, number))

    done = pl.pallas_call(
        functools.partial(kernel, groups, devs, leaves),
        out_shape=jax.ShapeDtypeStruct((2, 8, LANES), jnp.float32),
        in_specs=[hbm] * 5,
        out_specs=vmem,
        scratch_shapes=[
            pltpu.VMEM((rows, features), jnp.int32),
            pltpu.VMEM((1, leaves), jnp.int32),
            pltpu.VMEM((rows // LANES, LANES), jnp.bfloat16),
            pltpu.VMEM((rows // LANES, LANES), jnp.bfloat16),
            pltpu.VMEM((rows // LANES, LANES), jnp.int32),
            pltpu.VMEM((3, rows // LANES, LANES), jnp.float32),
            pltpu.SemaphoreType.DMA((rows // STEP_ROWS,)),
            pltpu.SemaphoreType.DMA((4,)),
            pltpu.VMEM((features, rows), jnp.float32),
            pltpu.VMEM((LANES, rows), jnp.bfloat16),
            floats(2, 2 * planes, quads, groups),
            floats(2 * planes, quads, groups),
            floats(relayed, half, groups),
            floats(relayed, half),
            floats(relayed, half),
            floats(relayed, half),
            floats(relayed, half),
            floats(relayed, quads),
            floats(relayed, quads),
            floats(2, 4, quads),
            pltpu.VMEM((8, LANES), jnp.float32),
            pltpu.VMEM((8, LANES), jnp.float32),
            pltpu.VMEM((everyone, 1, LANES), jnp.float32),
            sems(2 * planes),
            sems(relayed),
            sems(relayed),
            sems(relayed),
            sems(relayed),
            sems(relayed),
            sems(relayed),
            sems(8),
            sems(1),
            sems(everyone),
        ],
        compiler_params=pltpu.CompilerParams(
            collective_id=0, has_side_effects=True, vmem_limit_bytes=63 * 1024 * 1024
        ),
    )(
        bin_index, gradient.reshape(rows // LANES, LANES), hessian.reshape(rows // LANES, LANES),
        child_id.reshape(rows // LANES, LANES), smaller_side.reshape(1, leaves),
    )
    gain, best = pl.pallas_call(
        finish,
        out_shape=(
            jax.ShapeDtypeStruct((per_dev, own_leaves), jnp.float32),
            jax.ShapeDtypeStruct((own_leaves,), jnp.float32),
        ),
        in_specs=[vmem],
        out_specs=(vmem, vmem),
    )(done)
    return (gain.T, best)


def fits(groups, devs, leaves, features, rows):
    planes = devs // 4
    if groups != 2 or devs % 4 or planes != 4 or leaves != 32:
        return False
    return features == 8 * devs and rows % KCHUNK == 0


def solution(mesh):
    in_specs = (
        P(("group", "dev"), None),
        P(("group", "dev")),
        P(("group", "dev")),
        P(("group", "dev")),
        P(),
    )
    out_specs = (P("group", "dev"), P("group"))
    groups, devs = mesh.shape["group"], mesh.shape["dev"]

    def body(bin_index, gradient, hessian, child_id, smaller_side):
        rows, features = bin_index.shape
        args = (bin_index, gradient, hessian, child_id, smaller_side)
        if fits(groups, devs, smaller_side.shape[0], features, rows):
            return kernel_body(groups, devs, *args)
        return plain_body(*args)

    return jax.shard_map(body, mesh=mesh, in_specs=in_specs, out_specs=out_specs, check_vma=False)
```

```python
import functools

import jax
import jax.numpy as jnp
from jax import lax
from jax.experimental import pallas as pl
from jax.experimental.pallas import tpu as pltpu
from jax.sharding import PartitionSpec as P

BINS = 64
LANES = 128
KCHUNK = 1024
STEP_ROWS = 1024


reg_lambda = 1.0


def split_gains(hist_grad, hist_hess):
    left_grad = jnp.cumsum(hist_grad, axis=-1)[..., :-1]
    left_hess = jnp.cumsum(hist_hess, axis=-1)[..., :-1]
    total_grad = jnp.sum(hist_grad, axis=-1, keepdims=True)
    total_hess = jnp.sum(hist_hess, axis=-1, keepdims=True)
    right_grad = total_grad - left_grad
    value = left_grad * left_grad / (left_hess + reg_lambda)
    value = value + right_grad * right_grad / (total_hess - left_hess + reg_lambda)
    value = value - total_grad * total_grad / (total_hess + reg_lambda)
    return jnp.max(value, axis=-1)


def plain_body(bin_index, gradient, hessian, child_id, smaller_side):
    leaves = smaller_side.shape[0]
    features = bin_index.shape[1]
    target = 2 * jnp.arange(leaves, dtype=jnp.int32)[None, :] + smaller_side[None, :]
    chosen = child_id[:, None] == target
    nothing = jnp.zeros((), jnp.bfloat16)
    weights = jnp.concatenate(
        [
            jnp.where(chosen, gradient[:, None], nothing),
            jnp.where(chosen, hessian[:, None], nothing),
        ],
        axis=1,
    )
    levels = jnp.arange(BINS, dtype=jnp.int32)

    def one_feature(column):
        onehot = (column[:, None] == levels[None, :]).astype(jnp.bfloat16)
        product = lax.dot_general(
            weights, onehot, (((0,), (0,)), ((), ())), preferred_element_type=jnp.float32
        )
        return product.reshape(2, leaves, BINS).transpose(1, 0, 2).reshape(leaves, 2 * BINS)

    stacked = lax.map(one_feature, bin_index.T)
    owned = lax.psum_scatter(stacked, "dev", scatter_dimension=0, tiled=True)
    owned = lax.psum_scatter(owned, "group", scatter_dimension=1, tiled=True)
    hist_grad = owned[:, :, :BINS].transpose(1, 0, 2)
    hist_hess = owned[:, :, BINS:].transpose(1, 0, 2)
    best_gain = split_gains(hist_grad, hist_hess)
    child_best = lax.pmax(jnp.max(best_gain, axis=1), "dev")
    return (best_gain, child_best)


def kernel(
    groups, devs, leaves,
    bins_ref, grad_ref, hess_ref, child_ref, side_ref,
    done_ref,
    bins_v, side_v, grad_v, hess_v, child_v, values, bins_sem, small_sem,
    bins_t, weights, out, pair_in, a_in, b_in, c_in, d_in, e_in, f_out, f_in, near_in,
    gain_out, gain_in, best_in,
    pair_sem, a_sem, b_sem, c_sem, d_sem, e_sem, f_sem, near_sem, gain_sem, best_sem,
):
    rows, features = bins_ref.shape
    per_dev = features // devs
    own_features = per_dev // groups
    own_leaves = leaves // groups
    width = 2 * leaves
    slots = LANES // width
    quads = own_features // slots
    half = quads // 2
    planes = devs // 4
    last = planes - 1
    relayed = last - 1
    me_g = lax.axis_index("group")
    me_d = lax.axis_index("dev")
    me_c = lax.rem(me_d, 2)
    me_j = lax.div(me_d, 2)
    me_x = lax.rem(me_j, 2)
    me_z = lax.div(me_j, 2)
    barrier = pltpu.get_barrier_semaphore()
    step_rows = STEP_ROWS
    everyone = groups * devs

    def bins_copy(number):
        here = pl.ds(pl.multiple_of(number * step_rows, step_rows), step_rows)
        return pltpu.make_async_copy(bins_ref.at[here, :], bins_v.at[here, :], bins_sem.at[number])

    small = [
        pltpu.make_async_copy(source, place, small_sem.at[number])
        for number, (source, place) in enumerate(
            [(side_ref, side_v), (child_ref, child_v), (grad_ref, grad_v), (hess_ref, hess_v)]
        )
    ]
    for copy in small:
        copy.start()

    def start_bins(number, carry):
        bins_copy(number).start()
        return carry

    lax.fori_loop(0, rows // step_rows, start_bins, 0)

    def at(g, d):
        return {"group": g, "dev": d}

    def nth(step):
        other = lax.rem(me_g * devs + me_d + step, everyone)
        return at(lax.div(other, devs), lax.rem(other, devs))

    def greet(step, carry):
        pl.semaphore_signal(barrier, inc=1, device_id=nth(step), device_id_type=pl.DeviceIdType.MESH)
        return carry

    lax.fori_loop(1, everyone, greet, 0)

    pair_row = lax.broadcasted_iota(jnp.int32, (leaves, leaves), 0)
    pair_lane = lax.broadcasted_iota(jnp.int32, (leaves, leaves), 1)

    for copy in small:
        copy.wait()

    side = jnp.where(pair_lane == pair_row, side_v[...].astype(jnp.float32), 0.0)
    target = jnp.sum(side, axis=1, keepdims=True) + 2.0 * pair_row[:, :1].astype(jnp.float32)
    target = jnp.broadcast_to(target, (leaves, LANES)).astype(jnp.bfloat16)
    values[0] = grad_v[...].astype(jnp.float32)
    values[1] = hess_v[...].astype(jnp.float32)
    values[2] = child_v[...].astype(jnp.float32)
    no_weight = jnp.zeros((), jnp.bfloat16)

    def prepare(number, carry):
        here = pl.ds(pl.multiple_of(number * step_rows, step_rows), step_rows)
        for piece in range(step_rows // LANES):
            row = number * (step_rows // LANES) + piece
            there = pl.ds(pl.multiple_of(row * LANES, LANES), LANES)

            def spread(kind):
                return jnp.broadcast_to(values[kind, pl.ds(row, 1), :], (leaves, LANES)).astype(jnp.bfloat16)

            chosen = spread(2) == target
            for kind in range(2):
                value = jnp.where(chosen, spread(kind), no_weight)
                for s in range(slots):
                    start = s * width + kind * leaves
                    weights[start:start + leaves, there] = value
        return carry

    def turn_bins(number, carry):
        here = pl.ds(pl.multiple_of(number * step_rows, step_rows), step_rows)
        bins_copy(number).wait()
        bins_t[:, here] = bins_v[here, :].astype(jnp.float32).astype(jnp.bfloat16).T.astype(jnp.float32)
        return carry

    lax.fori_loop(0, rows // step_rows, prepare, 0)
    lax.fori_loop(0, rows // step_rows, turn_bins, 0)

    chunk = min(rows, KCHUNK)
    pack = 16
    level = lax.broadcasted_iota(jnp.int32, (pack, chunk), 0).astype(jnp.float32).astype(jnp.bfloat16)
    one = jnp.ones((), jnp.bfloat16)
    zero = jnp.zeros((), jnp.bfloat16)
    lane = lax.broadcasted_iota(jnp.int32, (BINS, LANES), 1)

    def block(d):
        base = pl.multiple_of(d * per_dev, per_dev)
        total = None
        for start in range(0, rows, chunk):
            parts = []
            levels = bins_t[pl.ds(base, per_dev), start:start + chunk]
            for f in range(per_dev):
                row = jnp.broadcast_to(levels[f:f + 1, :], (pack, chunk)).astype(jnp.bfloat16)
                for low in range(0, BINS, pack):
                    parts.append(jnp.where(row <= level + jnp.bfloat16(low), one, zero))
            below = jnp.concatenate(parts, axis=0)
            product = lax.dot_general(
                below, weights[:, start:start + chunk], (((1,), (1,)), ((), ())),
                preferred_element_type=jnp.float32,
            )
            total = product if total is None else total + product
        result = []
        for y in range(groups):
            for q in range(quads):
                piece = None
                for s in range(slots):
                    f = (y * quads + q) * slots + s
                    here = total[f * BINS:(f + 1) * BINS, :]
                    piece = here if piece is None else jnp.where(lane >= s * width, here, piece)
                result.append((y, q, piece))
        return result

    def remote(source, place, sem, index, device):
        return pltpu.make_async_remote_copy(
            src_ref=source, dst_ref=place, send_sem=sem.at[0, index], recv_sem=sem.at[1, index],
            device_id=device, device_id_type=pl.DeviceIdType.MESH,
        )

    def pick(index, choices):
        result = choices[-1]
        for number in range(len(choices) - 1):
            result = jnp.where(index == number, choices[number], result)
        return result

    def flipped(turn):
        result, bit = 0, 1
        while bit < planes:
            digit = lax.rem(lax.div(me_z, bit), 2)
            result = result + bit * (1 - digit if (turn // bit) % 2 else digit)
            bit *= 2
        return result

    planes_of = [flipped(last - k) for k in range(planes)]

    def plane(k):
        return planes_of[k] if isinstance(k, int) else pick(k, planes_of)

    def dev_of(k, dx, core):
        x = jnp.where(dx == 1, 1 - me_x, me_x)
        return (plane(k) * 2 + x) * 2 + core

    pair_dev = at(me_g, me_j * 2 + 1 - me_c)
    x_dev_d = (me_z * 2 + 1 - me_x) * 2 + me_c
    x_dev = at(me_g, x_dev_d)
    y_g = 1 - me_g
    y_dev = at(y_g, me_d)
    diag_dev = at(y_g, x_dev_d)

    def pair_copy(n):
        return remote(out.at[0, n], pair_in.at[n], pair_sem, n, pair_dev)

    first = slice(0, half)
    second = slice(half, quads)

    def a_copy(k):
        return remote(out.at[1, 2 * k + 1, first], a_in.at[k], a_sem, k, x_dev)

    def b_copy(k):
        return remote(out.at[1, 2 * k + 1, second, me_g], b_in.at[k], b_sem, k, x_dev)

    def c_copy(k):
        return remote(out.at[1, 2 * k + 1, second, y_g], c_in.at[k], c_sem, k, y_dev)

    def d_copy(k):
        return remote(out.at[1, 2 * k, second, y_g], d_in.at[k], d_sem, k, y_dev)

    def e_copy(k):
        return remote(out.at[1, 2 * k, first, y_g], e_in.at[k], e_sem, k, y_dev)

    def f_copy(k):
        d = (plane(k) * 2 + me_x) * 2 + me_c
        return remote(f_out.at[k], f_in.at[k], f_sem, k, at(me_g, d))

    def direct_copy(k, n):
        dx, y = ((1, y_g), (1, me_g), (0, y_g), (0, me_g))[n]
        d = dev_of(k, dx, me_c)
        return remote(out.at[1, 2 * k + dx, :, y], near_in.at[k - relayed, n], near_sem, (k - relayed) * 4 + n, at(y, d))

    def direct(k):
        return range(3 if k == last else 4)

    def do_b(k):
        c_copy(k).wait_recv()
        out[1, 2 * k + 1, second, me_g] = out[1, 2 * k + 1, second, me_g] + c_in[k]
        b_copy(k).start()

    def do_e(k):
        a_copy(k).wait_recv()
        out[1, 2 * k, first, y_g] = out[1, 2 * k, first, y_g] + a_in[k, :, y_g]
        e_copy(k).start()

    def do_f(k):
        b_copy(k).wait_recv()
        d_copy(k).wait_recv()
        f_out[k, second] = out[1, 2 * k, second, me_g] + b_in[k] + d_in[k]
        e_copy(k).wait_recv()
        f_out[k, first] = out[1, 2 * k, first, me_g] + a_in[k, :, me_g] + e_in[k]
        f_copy(k).start()

    steps = [(k, 1) for k in range(last)] + [(k, 0) for k in range(last)] + [(last, 1), (last, 0)]
    turns = len(steps)

    def group_of(step):
        k = pick(step, [a for a, _ in steps])
        dx = pick(step, [a for _, a in steps])
        return k, dx, 2 * k + dx

    def work(step, is_p):
        k, dx, n = group_of(step)
        role = jnp.where(is_p, 0, 1)
        for y, q, piece in block(dev_of(k, dx, jnp.where(is_p, 1 - me_c, me_c))):
            out[role, n, q, y] = piece

    def pass_on(step):
        k, dx, n = group_of(step)
        pair_copy(n).wait_recv()
        out[1, n] = out[1, n] + pair_in[n]

        @pl.when(k < relayed)
        def _():
            @pl.when(dx == 1)
            def _():
                a_copy(k).start()
                c_copy(k).start()

            @pl.when(dx == 0)
            def _():
                d_copy(k).start()
                do_e(k)
                do_b(k)

        @pl.when(k >= relayed)
        def _():
            @pl.when(dx == 1)
            def _():
                direct_copy(k, 0).start()
                direct_copy(k, 1).start()

            @pl.when(dx == 0)
            def _():
                direct_copy(k, 2).start()

                @pl.when(k < last)
                def _():
                    direct_copy(k, 3).start()

    def iteration(turn, carry):
        step = lax.div(turn, 2) * 2
        is_p = lax.rem(turn, 2) == 0
        work(step, is_p)
        work(step + 1, is_p)

        @pl.when(turn == 0)
        def _():
            pl.semaphore_wait(barrier, everyone - 1)

        @pl.when(is_p)
        def _():
            pair_copy(group_of(step)[2]).start()
            pair_copy(group_of(step + 1)[2]).start()

        @pl.when(jnp.logical_not(is_p))
        def _():
            for k in range(relayed - 1):
                @pl.when(turn == turns - 1 - 2 * (relayed - 1 - k))
                def _():
                    do_f(k)

            pass_on(step)
            pass_on(step + 1)

        return carry

    lax.fori_loop(0, turns - 2, iteration, 0)

    def closing(slot, carry):
        step = turns - 2 + lax.div(slot, 2)
        is_p = lax.rem(slot, 2) == 0
        work(step, is_p)

        @pl.when(is_p)
        def _():
            pair_copy(group_of(step)[2]).start()

        @pl.when(jnp.logical_not(is_p))
        def _():
            pass_on(step)

        @pl.when(slot == 2)
        def _():
            do_f(relayed - 1)

        return carry

    lax.fori_loop(0, 4, closing, 0)

    hist = out[1, 2 * last, :, me_g]
    for k in range(relayed):
        f_copy(k).wait_recv()
        hist = hist + f_in[k]
    for k in range(relayed, planes):
        for number in direct(k):
            direct_copy(k, number).wait_recv()
            hist = hist + near_in[k - relayed, number]

    usable = lax.rem(lane, width) < leaves
    keep = lax.broadcasted_iota(jnp.int32, (BINS, LANES), 0) < BINS - 1
    lane8 = lax.broadcasted_iota(jnp.int32, (8, LANES), 1)
    row8 = lax.broadcasted_iota(jnp.int32, (8, LANES), 0)
    tile = jnp.full((8, LANES), -jnp.inf, jnp.float32)
    for q in range(quads):
        left_grad = hist[q]
        left_hess = jnp.where(usable, pltpu.roll(left_grad, LANES - leaves, 1), 0.0)
        total_grad, total_hess = left_grad[BINS - 1:, :], left_hess[BINS - 1:, :]
        right_grad = total_grad - left_grad
        value = left_grad * left_grad / (left_hess + reg_lambda)
        value = value + right_grad * right_grad / (total_hess - left_hess + reg_lambda)
        value = value - total_grad * total_grad / (total_hess + reg_lambda)
        value = jnp.where(keep, value, -jnp.inf)
        best = jnp.broadcast_to(jnp.max(value, axis=0, keepdims=True), (8, LANES))
        for s in range(slots):
            moved = pltpu.roll(best, LANES - s * width, 1) if s else best
            tile = jnp.where(row8 == q * slots + s, moved, tile)
    top = jnp.max(tile, axis=0, keepdims=True)
    tile = jnp.where(row8 == 7, top, tile)
    gain_out[...] = tile

    gain_copy = remote(gain_out, gain_in, gain_sem, 0, y_dev)
    gain_copy.start()

    def best_copy(step):
        return remote(gain_out.at[pl.ds(7, 1)], best_in.at[step], best_sem, step, nth(step))

    for step in range(1, everyone):
        if step != devs:
            best_copy(step).start()
    for n in range(2 * planes):
        pair_copy(n).wait_send()
    for k in range(relayed):
        for make in (a_copy, b_copy, c_copy, d_copy, e_copy, f_copy):
            make(k).wait_send()
    for k in range(relayed, planes):
        for number in direct(k):
            direct_copy(k, number).wait_send()
    gain_copy.wait()
    other = gain_in[...]
    top = jnp.maximum(top, other[7:8, :])
    low_tile = jnp.where(me_g == 0, tile, other)
    high_tile = jnp.where(me_g == 0, other, tile)
    gain = jnp.where(row8 < own_features, low_tile, pltpu.roll(high_tile, own_features, 0))
    done_ref[0] = jnp.where(me_g == 0, gain, pltpu.roll(gain, LANES - own_leaves, 1))
    for step in range(1, everyone):
        if step != devs:
            best_copy(step).wait()
            top = jnp.maximum(top, best_in[step])
    top = jnp.broadcast_to(top, (8, LANES))
    done_ref[1] = jnp.where(me_g == 0, top, pltpu.roll(top, LANES - own_leaves, 1))


def finish(done_ref, gain_ref, best_ref):
    gain_ref[...] = done_ref[0, :gain_ref.shape[0], :gain_ref.shape[1]]
    best_ref[...] = done_ref[1, 0, :best_ref.shape[0]]


def kernel_body(groups, devs, bin_index, gradient, hessian, child_id, smaller_side):
    rows, features = bin_index.shape
    leaves = smaller_side.shape[0]
    per_dev = features // devs
    own_features = per_dev // groups
    own_leaves = leaves // groups
    slots = LANES // (2 * leaves)
    quads = own_features // slots
    half = quads // 2
    planes = devs // 4
    relayed = planes - 2
    everyone = groups * devs
    vmem = pl.BlockSpec(memory_space=pltpu.VMEM)
    hbm = pl.BlockSpec(memory_space=pltpu.HBM)

    def floats(*shape):
        return pltpu.VMEM(shape + (BINS, LANES), jnp.float32)

    def sems(number):
        return pltpu.SemaphoreType.DMA((2, number))

    done = pl.pallas_call(
        functools.partial(kernel, groups, devs, leaves),
        out_shape=jax.ShapeDtypeStruct((2, 8, LANES), jnp.float32),
        in_specs=[hbm] * 5,
        out_specs=vmem,
        scratch_shapes=[
            pltpu.VMEM((rows, features), jnp.int32),
            pltpu.VMEM((1, leaves), jnp.int32),
            pltpu.VMEM((rows // LANES, LANES), jnp.bfloat16),
            pltpu.VMEM((rows // LANES, LANES), jnp.bfloat16),
            pltpu.VMEM((rows // LANES, LANES), jnp.int32),
            pltpu.VMEM((3, rows // LANES, LANES), jnp.float32),
            pltpu.SemaphoreType.DMA((rows // STEP_ROWS,)),
            pltpu.SemaphoreType.DMA((4,)),
            pltpu.VMEM((features, rows), jnp.float32),
            pltpu.VMEM((LANES, rows), jnp.bfloat16),
            floats(2, 2 * planes, quads, groups),
            floats(2 * planes, quads, groups),
            floats(relayed, half, groups),
            floats(relayed, half),
            floats(relayed, half),
            floats(relayed, half),
            floats(relayed, half),
            floats(relayed, quads),
            floats(relayed, quads),
            floats(2, 4, quads),
            pltpu.VMEM((8, LANES), jnp.float32),
            pltpu.VMEM((8, LANES), jnp.float32),
            pltpu.VMEM((everyone, 1, LANES), jnp.float32),
            sems(2 * planes),
            sems(relayed),
            sems(relayed),
            sems(relayed),
            sems(relayed),
            sems(relayed),
            sems(relayed),
            sems(8),
            sems(1),
            sems(everyone),
        ],
        compiler_params=pltpu.CompilerParams(
            collective_id=0, has_side_effects=True, vmem_limit_bytes=63 * 1024 * 1024
        ),
    )(
        bin_index, gradient.reshape(rows // LANES, LANES), hessian.reshape(rows // LANES, LANES),
        child_id.reshape(rows // LANES, LANES), smaller_side.reshape(1, leaves),
    )
    gain, best = pl.pallas_call(
        finish,
        out_shape=(
            jax.ShapeDtypeStruct((per_dev, own_leaves), jnp.float32),
            jax.ShapeDtypeStruct((own_leaves,), jnp.float32),
        ),
        in_specs=[vmem],
        out_specs=(vmem, vmem),
    )(done)
    return (gain.T, best)


def fits(groups, devs, leaves, features, rows):
    planes = devs // 4
    if groups != 2 or devs % 4 or planes != 4 or leaves != 32:
        return False
    return features == 8 * devs and rows % KCHUNK == 0


def solution(mesh):
    in_specs = (
        P(("group", "dev"), None),
        P(("group", "dev")),
        P(("group", "dev")),
        P(("group", "dev")),
        P(),
    )
    out_specs = (P("group", "dev"), P("group"))
    groups, devs = mesh.shape["group"], mesh.shape["dev"]

    def body(bin_index, gradient, hessian, child_id, smaller_side):
        rows, features = bin_index.shape
        args = (bin_index, gradient, hessian, child_id, smaller_side)
        if fits(groups, devs, smaller_side.shape[0], features, rows):
            return kernel_body(groups, devs, *args)
        return plain_body(*args)

    return jax.shard_map(body, mesh=mesh, in_specs=in_specs, out_specs=out_specs, check_vma=False)
```

```python
import functools

import jax
import jax.numpy as jnp
from jax import lax
from jax.experimental import pallas as pl
from jax.experimental.pallas import tpu as pltpu
from jax.sharding import PartitionSpec as P

BINS = 64
LANES = 128
KCHUNK = 1024
STEP_ROWS = 1024


reg_lambda = 1.0


def split_gains(hist_grad, hist_hess):
    left_grad = jnp.cumsum(hist_grad, axis=-1)[..., :-1]
    left_hess = jnp.cumsum(hist_hess, axis=-1)[..., :-1]
    total_grad = jnp.sum(hist_grad, axis=-1, keepdims=True)
    total_hess = jnp.sum(hist_hess, axis=-1, keepdims=True)
    right_grad = total_grad - left_grad
    value = left_grad * left_grad / (left_hess + reg_lambda)
    value = value + right_grad * right_grad / (total_hess - left_hess + reg_lambda)
    value = value - total_grad * total_grad / (total_hess + reg_lambda)
    return jnp.max(value, axis=-1)


def plain_body(bin_index, gradient, hessian, child_id, smaller_side):
    leaves = smaller_side.shape[0]
    features = bin_index.shape[1]
    target = 2 * jnp.arange(leaves, dtype=jnp.int32)[None, :] + smaller_side[None, :]
    chosen = child_id[:, None] == target
    nothing = jnp.zeros((), jnp.bfloat16)
    weights = jnp.concatenate(
        [
            jnp.where(chosen, gradient[:, None], nothing),
            jnp.where(chosen, hessian[:, None], nothing),
        ],
        axis=1,
    )
    levels = jnp.arange(BINS, dtype=jnp.int32)

    def one_feature(column):
        onehot = (column[:, None] == levels[None, :]).astype(jnp.bfloat16)
        product = lax.dot_general(
            weights, onehot, (((0,), (0,)), ((), ())), preferred_element_type=jnp.float32
        )
        return product.reshape(2, leaves, BINS).transpose(1, 0, 2).reshape(leaves, 2 * BINS)

    stacked = lax.map(one_feature, bin_index.T)
    owned = lax.psum_scatter(stacked, "dev", scatter_dimension=0, tiled=True)
    owned = lax.psum_scatter(owned, "group", scatter_dimension=1, tiled=True)
    hist_grad = owned[:, :, :BINS].transpose(1, 0, 2)
    hist_hess = owned[:, :, BINS:].transpose(1, 0, 2)
    best_gain = split_gains(hist_grad, hist_hess)
    child_best = lax.pmax(jnp.max(best_gain, axis=1), "dev")
    return (best_gain, child_best)


def kernel(
    groups, devs, leaves,
    bins_ref, grad_ref, hess_ref, child_ref, side_ref,
    done_ref,
    bins_v, side_v, grad_v, hess_v, child_v, values, bins_sem, small_sem,
    bins_t, weights, out, pair_in, a_in, b_in, c_in, d_in, e_in, f_out, f_in, near_in,
    gain_out, gain_in, best_in,
    pair_sem, a_sem, b_sem, c_sem, d_sem, e_sem, f_sem, near_sem, gain_sem, best_sem,
):
    rows, features = bins_ref.shape
    per_dev = features // devs
    own_features = per_dev // groups
    own_leaves = leaves // groups
    width = 2 * leaves
    slots = LANES // width
    quads = own_features // slots
    half = quads // 2
    planes = devs // 4
    last = planes - 1
    relayed = last - 1
    me_g = lax.axis_index("group")
    me_d = lax.axis_index("dev")
    me_c = lax.rem(me_d, 2)
    me_j = lax.div(me_d, 2)
    me_x = lax.rem(me_j, 2)
    me_z = lax.div(me_j, 2)
    barrier = pltpu.get_barrier_semaphore()
    step_rows = STEP_ROWS
    everyone = groups * devs

    def bins_copy(number):
        here = pl.ds(pl.multiple_of(number * step_rows, step_rows), step_rows)
        return pltpu.make_async_copy(bins_ref.at[here, :], bins_v.at[here, :], bins_sem.at[number])

    small = [
        pltpu.make_async_copy(source, place, small_sem.at[number])
        for number, (source, place) in enumerate(
            [(side_ref, side_v), (child_ref, child_v), (grad_ref, grad_v), (hess_ref, hess_v)]
        )
    ]
    for copy in small:
        copy.start()

    def start_bins(number, carry):
        bins_copy(number).start()
        return carry

    lax.fori_loop(0, rows // step_rows, start_bins, 0)

    def at(g, d):
        return {"group": g, "dev": d}

    def nth(step):
        other = lax.rem(me_g * devs + me_d + step, everyone)
        return at(lax.div(other, devs), lax.rem(other, devs))

    def greet(step, carry):
        pl.semaphore_signal(barrier, inc=1, device_id=nth(step), device_id_type=pl.DeviceIdType.MESH)
        return carry

    lax.fori_loop(1, everyone, greet, 0)

    pair_row = lax.broadcasted_iota(jnp.int32, (leaves, leaves), 0)
    pair_lane = lax.broadcasted_iota(jnp.int32, (leaves, leaves), 1)

    for copy in small:
        copy.wait()

    side = jnp.where(pair_lane == pair_row, side_v[...].astype(jnp.float32), 0.0)
    target = jnp.sum(side, axis=1, keepdims=True) + 2.0 * pair_row[:, :1].astype(jnp.float32)
    target = jnp.broadcast_to(target, (leaves, LANES)).astype(jnp.bfloat16)
    values[0] = grad_v[...].astype(jnp.float32)
    values[1] = hess_v[...].astype(jnp.float32)
    values[2] = child_v[...].astype(jnp.float32)
    no_weight = jnp.zeros((), jnp.bfloat16)

    def prepare(number, carry):
        here = pl.ds(pl.multiple_of(number * step_rows, step_rows), step_rows)
        for piece in range(step_rows // LANES):
            row = number * (step_rows // LANES) + piece
            there = pl.ds(pl.multiple_of(row * LANES, LANES), LANES)

            def spread(kind):
                return jnp.broadcast_to(values[kind, pl.ds(row, 1), :], (leaves, LANES)).astype(jnp.bfloat16)

            chosen = spread(2) == target
            for kind in range(2):
                value = jnp.where(chosen, spread(kind), no_weight)
                for s in range(slots):
                    start = s * width + kind * leaves
                    weights[start:start + leaves, there] = value
        return carry

    def turn_bins(number, carry):
        here = pl.ds(pl.multiple_of(number * step_rows, step_rows), step_rows)
        bins_copy(number).wait()
        bins_t[:, here] = bins_v[here, :].astype(jnp.float32).astype(jnp.bfloat16).T.astype(jnp.float32)
        return carry

    lax.fori_loop(0, rows // step_rows, prepare, 0)
    lax.fori_loop(0, rows // step_rows, turn_bins, 0)

    chunk = min(rows, KCHUNK)
    pack = 16
    level = lax.broadcasted_iota(jnp.int32, (pack, chunk), 0).astype(jnp.float32).astype(jnp.bfloat16)
    one = jnp.ones((), jnp.bfloat16)
    zero = jnp.zeros((), jnp.bfloat16)
    lane = lax.broadcasted_iota(jnp.int32, (BINS, LANES), 1)

    def block(d):
        base = pl.multiple_of(d * per_dev, per_dev)
        total = None
        for start in range(0, rows, chunk):
            parts = []
            levels = bins_t[pl.ds(base, per_dev), start:start + chunk]
            for f in range(per_dev):
                row = jnp.broadcast_to(levels[f:f + 1, :], (pack, chunk)).astype(jnp.bfloat16)
                for low in range(0, BINS, pack):
                    parts.append(jnp.where(row <= level + jnp.bfloat16(low), one, zero))
            below = jnp.concatenate(parts, axis=0)
            product = lax.dot_general(
                below, weights[:, start:start + chunk], (((1,), (1,)), ((), ())),
                preferred_element_type=jnp.float32,
            )
            total = product if total is None else total + product
        result = []
        for y in range(groups):
            for q in range(quads):
                piece = None
                for s in range(slots):
                    f = (y * quads + q) * slots + s
                    here = total[f * BINS:(f + 1) * BINS, :]
                    piece = here if piece is None else jnp.where(lane >= s * width, here, piece)
                result.append((y, q, piece))
        return result

    def remote(source, place, sem, index, device):
        return pltpu.make_async_remote_copy(
            src_ref=source, dst_ref=place, send_sem=sem.at[0, index], recv_sem=sem.at[1, index],
            device_id=device, device_id_type=pl.DeviceIdType.MESH,
        )

    def pick(index, choices):
        result = choices[-1]
        for number in range(len(choices) - 1):
            result = jnp.where(index == number, choices[number], result)
        return result

    def flipped(turn):
        result, bit = 0, 1
        while bit < planes:
            digit = lax.rem(lax.div(me_z, bit), 2)
            result = result + bit * (1 - digit if (turn // bit) % 2 else digit)
            bit *= 2
        return result

    planes_of = [flipped(last - k) for k in range(planes)]

    def plane(k):
        return planes_of[k] if isinstance(k, int) else pick(k, planes_of)

    def dev_of(k, dx, core):
        x = jnp.where(dx == 1, 1 - me_x, me_x)
        return (plane(k) * 2 + x) * 2 + core

    pair_dev = at(me_g, me_j * 2 + 1 - me_c)
    x_dev_d = (me_z * 2 + 1 - me_x) * 2 + me_c
    x_dev = at(me_g, x_dev_d)
    y_g = 1 - me_g
    y_dev = at(y_g, me_d)
    diag_dev = at(y_g, x_dev_d)

    def pair_copy(n):
        return remote(out.at[0, n], pair_in.at[n], pair_sem, n, pair_dev)

    first = slice(0, half)
    second = slice(half, quads)

    def a_copy(k):
        return remote(out.at[1, 2 * k + 1, first], a_in.at[k], a_sem, k, x_dev)

    def b_copy(k):
        return remote(out.at[1, 2 * k + 1, second, me_g], b_in.at[k], b_sem, k, x_dev)

    def c_copy(k):
        return remote(out.at[1, 2 * k + 1, second, y_g], c_in.at[k], c_sem, k, y_dev)

    def d_copy(k):
        return remote(out.at[1, 2 * k, second, y_g], d_in.at[k], d_sem, k, y_dev)

    def e_copy(k):
        return remote(out.at[1, 2 * k, first, y_g], e_in.at[k], e_sem, k, y_dev)

    def f_copy(k):
        d = (plane(k) * 2 + me_x) * 2 + me_c
        return remote(f_out.at[k], f_in.at[k], f_sem, k, at(me_g, d))

    def direct_copy(k, n):
        dx, y = ((1, y_g), (1, me_g), (0, y_g), (0, me_g))[n]
        d = dev_of(k, dx, me_c)
        return remote(out.at[1, 2 * k + dx, :, y], near_in.at[k - relayed, n], near_sem, (k - relayed) * 4 + n, at(y, d))

    def direct(k):
        return range(3 if k == last else 4)

    def do_b(k):
        c_copy(k).wait_recv()
        out[1, 2 * k + 1, second, me_g] = out[1, 2 * k + 1, second, me_g] + c_in[k]
        b_copy(k).start()

    def do_e(k):
        a_copy(k).wait_recv()
        out[1, 2 * k, first, y_g] = out[1, 2 * k, first, y_g] + a_in[k, :, y_g]
        e_copy(k).start()

    def do_f(k):
        b_copy(k).wait_recv()
        d_copy(k).wait_recv()
        f_out[k, second] = out[1, 2 * k, second, me_g] + b_in[k] + d_in[k]
        e_copy(k).wait_recv()
        f_out[k, first] = out[1, 2 * k, first, me_g] + a_in[k, :, me_g] + e_in[k]
        f_copy(k).start()

    steps = [(k, 1) for k in range(last)] + [(k, 0) for k in range(last)] + [(last, 1), (last, 0)]
    turns = len(steps)

    def group_of(step):
        k = pick(step, [a for a, _ in steps])
        dx = pick(step, [a for _, a in steps])
        return k, dx, 2 * k + dx

    def work(step, is_p):
        k, dx, n = group_of(step)
        role = jnp.where(is_p, 0, 1)
        for y, q, piece in block(dev_of(k, dx, jnp.where(is_p, 1 - me_c, me_c))):
            out[role, n, q, y] = piece

    def pass_on(step):
        k, dx, n = group_of(step)
        pair_copy(n).wait_recv()
        out[1, n] = out[1, n] + pair_in[n]

        @pl.when(k < relayed)
        def _():
            @pl.when(dx == 1)
            def _():
                a_copy(k).start()
                c_copy(k).start()

            @pl.when(dx == 0)
            def _():
                d_copy(k).start()
                do_e(k)
                do_b(k)

        @pl.when(k >= relayed)
        def _():
            @pl.when(dx == 1)
            def _():
                direct_copy(k, 0).start()
                direct_copy(k, 1).start()

            @pl.when(dx == 0)
            def _():
                direct_copy(k, 2).start()

                @pl.when(k < last)
                def _():
                    direct_copy(k, 3).start()

    def iteration(turn, carry):
        step = lax.div(turn, 2) * 2
        is_p = lax.rem(turn, 2) == 0
        work(step, is_p)
        work(step + 1, is_p)

        @pl.when(turn == 0)
        def _():
            pl.semaphore_wait(barrier, everyone - 1)

        @pl.when(is_p)
        def _():
            pair_copy(group_of(step)[2]).start()
            pair_copy(group_of(step + 1)[2]).start()

        @pl.when(jnp.logical_not(is_p))
        def _():
            for k in range(relayed - 1):
                @pl.when(turn == turns - 1 - 2 * (relayed - 1 - k))
                def _():
                    do_f(k)

            pass_on(step)
            pass_on(step + 1)

        return carry

    lax.fori_loop(0, turns - 2, iteration, 0)

    def closing(slot, carry):
        step = turns - 2 + lax.div(slot, 2)
        is_p = lax.rem(slot, 2) == 0
        work(step, is_p)

        @pl.when(is_p)
        def _():
            pair_copy(group_of(step)[2]).start()

        @pl.when(jnp.logical_not(is_p))
        def _():
            pass_on(step)

        @pl.when(slot == 2)
        def _():
            do_f(relayed - 1)

        return carry

    lax.fori_loop(0, 4, closing, 0)

    hist = out[1, 2 * last, :, me_g]
    for k in range(relayed):
        f_copy(k).wait_recv()
        hist = hist + f_in[k]
    for k in range(relayed, planes):
        for number in direct(k):
            direct_copy(k, number).wait_recv()
            hist = hist + near_in[k - relayed, number]

    usable = lax.rem(lane, width) < leaves
    keep = lax.broadcasted_iota(jnp.int32, (BINS, LANES), 0) < BINS - 1
    lane8 = lax.broadcasted_iota(jnp.int32, (8, LANES), 1)
    row8 = lax.broadcasted_iota(jnp.int32, (8, LANES), 0)
    tile = jnp.full((8, LANES), -jnp.inf, jnp.float32)
    for q in range(quads):
        left_grad = hist[q]
        left_hess = jnp.where(usable, pltpu.roll(left_grad, LANES - leaves, 1), 0.0)
        total_grad, total_hess = left_grad[BINS - 1:, :], left_hess[BINS - 1:, :]
        right_grad = total_grad - left_grad
        value = left_grad * left_grad / (left_hess + reg_lambda)
        value = value + right_grad * right_grad / (total_hess - left_hess + reg_lambda)
        value = value - total_grad * total_grad / (total_hess + reg_lambda)
        value = jnp.where(keep, value, -jnp.inf)
        best = jnp.broadcast_to(jnp.max(value, axis=0, keepdims=True), (8, LANES))
        for s in range(slots):
            moved = pltpu.roll(best, LANES - s * width, 1) if s else best
            tile = jnp.where(row8 == q * slots + s, moved, tile)
    top = jnp.max(tile, axis=0, keepdims=True)
    tile = jnp.where(row8 == 7, top, tile)
    gain_out[...] = tile

    gain_copy = remote(gain_out, gain_in, gain_sem, 0, y_dev)

    def best_copy(step):
        return remote(gain_out.at[pl.ds(7, 1)], best_in.at[step], best_sem, step, nth(step))

    for step in range(1, everyone):
        if step != devs:
            best_copy(step).start()
    gain_copy.start()
    for n in range(2 * planes):
        pair_copy(n).wait_send()
    for k in range(relayed):
        for make in (a_copy, b_copy, c_copy, d_copy, e_copy, f_copy):
            make(k).wait_send()
    for k in range(relayed, planes):
        for number in direct(k):
            direct_copy(k, number).wait_send()
    gain_copy.wait_recv()
    other = gain_in[...]
    top = jnp.maximum(top, other[7:8, :])
    low_tile = jnp.where(me_g == 0, tile, other)
    high_tile = jnp.where(me_g == 0, other, tile)
    gain = jnp.where(row8 < own_features, low_tile, pltpu.roll(high_tile, own_features, 0))
    done_ref[0] = jnp.where(me_g == 0, gain, pltpu.roll(gain, LANES - own_leaves, 1))
    for step in range(1, everyone):
        if step != devs:
            best_copy(step).wait_recv()
            top = jnp.maximum(top, best_in[step])
    top = jnp.broadcast_to(top, (8, LANES))
    done_ref[1] = jnp.where(me_g == 0, top, pltpu.roll(top, LANES - own_leaves, 1))
    gain_copy.wait_send()
    for step in range(1, everyone):
        if step != devs:
            best_copy(step).wait_send()


def finish(done_ref, gain_ref, best_ref):
    gain_ref[...] = done_ref[0, :gain_ref.shape[0], :gain_ref.shape[1]]
    best_ref[...] = done_ref[1, 0, :best_ref.shape[0]]


def kernel_body(groups, devs, bin_index, gradient, hessian, child_id, smaller_side):
    rows, features = bin_index.shape
    leaves = smaller_side.shape[0]
    per_dev = features // devs
    own_features = per_dev // groups
    own_leaves = leaves // groups
    slots = LANES // (2 * leaves)
    quads = own_features // slots
    half = quads // 2
    planes = devs // 4
    relayed = planes - 2
    everyone = groups * devs
    vmem = pl.BlockSpec(memory_space=pltpu.VMEM)
    hbm = pl.BlockSpec(memory_space=pltpu.HBM)

    def floats(*shape):
        return pltpu.VMEM(shape + (BINS, LANES), jnp.float32)

    def sems(number):
        return pltpu.SemaphoreType.DMA((2, number))

    done = pl.pallas_call(
        functools.partial(kernel, groups, devs, leaves),
        out_shape=jax.ShapeDtypeStruct((2, 8, LANES), jnp.float32),
        in_specs=[hbm] * 5,
        out_specs=vmem,
        scratch_shapes=[
            pltpu.VMEM((rows, features), jnp.int32),
            pltpu.VMEM((1, leaves), jnp.int32),
            pltpu.VMEM((rows // LANES, LANES), jnp.bfloat16),
            pltpu.VMEM((rows // LANES, LANES), jnp.bfloat16),
            pltpu.VMEM((rows // LANES, LANES), jnp.int32),
            pltpu.VMEM((3, rows // LANES, LANES), jnp.float32),
            pltpu.SemaphoreType.DMA((rows // STEP_ROWS,)),
            pltpu.SemaphoreType.DMA((4,)),
            pltpu.VMEM((features, rows), jnp.float32),
            pltpu.VMEM((LANES, rows), jnp.bfloat16),
            floats(2, 2 * planes, quads, groups),
            floats(2 * planes, quads, groups),
            floats(relayed, half, groups),
            floats(relayed, half),
            floats(relayed, half),
            floats(relayed, half),
            floats(relayed, half),
            floats(relayed, quads),
            floats(relayed, quads),
            floats(2, 4, quads),
            pltpu.VMEM((8, LANES), jnp.float32),
            pltpu.VMEM((8, LANES), jnp.float32),
            pltpu.VMEM((everyone, 1, LANES), jnp.float32),
            sems(2 * planes),
            sems(relayed),
            sems(relayed),
            sems(relayed),
            sems(relayed),
            sems(relayed),
            sems(relayed),
            sems(8),
            sems(1),
            sems(everyone),
        ],
        compiler_params=pltpu.CompilerParams(
            collective_id=0, has_side_effects=True, vmem_limit_bytes=63 * 1024 * 1024
        ),
    )(
        bin_index, gradient.reshape(rows // LANES, LANES), hessian.reshape(rows // LANES, LANES),
        child_id.reshape(rows // LANES, LANES), smaller_side.reshape(1, leaves),
    )
    gain, best = pl.pallas_call(
        finish,
        out_shape=(
            jax.ShapeDtypeStruct((per_dev, own_leaves), jnp.float32),
            jax.ShapeDtypeStruct((own_leaves,), jnp.float32),
        ),
        in_specs=[vmem],
        out_specs=(vmem, vmem),
    )(done)
    return (gain.T, best)


def fits(groups, devs, leaves, features, rows):
    planes = devs // 4
    if groups != 2 or devs % 4 or planes != 4 or leaves != 32:
        return False
    return features == 8 * devs and rows % KCHUNK == 0


def solution(mesh):
    in_specs = (
        P(("group", "dev"), None),
        P(("group", "dev")),
        P(("group", "dev")),
        P(("group", "dev")),
        P(),
    )
    out_specs = (P("group", "dev"), P("group"))
    groups, devs = mesh.shape["group"], mesh.shape["dev"]

    def body(bin_index, gradient, hessian, child_id, smaller_side):
        rows, features = bin_index.shape
        args = (bin_index, gradient, hessian, child_id, smaller_side)
        if fits(groups, devs, smaller_side.shape[0], features, rows):
            return kernel_body(groups, devs, *args)
        return plain_body(*args)

    return jax.shard_map(body, mesh=mesh, in_specs=in_specs, out_specs=out_specs, check_vma=False)
```

```python
import functools

import jax
import jax.numpy as jnp
from jax import lax
from jax.experimental import pallas as pl
from jax.experimental.pallas import tpu as pltpu
from jax.sharding import PartitionSpec as P

BINS = 64
LANES = 128
KCHUNK = 1024
STEP_ROWS = 2048


reg_lambda = 1.0


def split_gains(hist_grad, hist_hess):
    left_grad = jnp.cumsum(hist_grad, axis=-1)[..., :-1]
    left_hess = jnp.cumsum(hist_hess, axis=-1)[..., :-1]
    total_grad = jnp.sum(hist_grad, axis=-1, keepdims=True)
    total_hess = jnp.sum(hist_hess, axis=-1, keepdims=True)
    right_grad = total_grad - left_grad
    value = left_grad * left_grad / (left_hess + reg_lambda)
    value = value + right_grad * right_grad / (total_hess - left_hess + reg_lambda)
    value = value - total_grad * total_grad / (total_hess + reg_lambda)
    return jnp.max(value, axis=-1)


def plain_body(bin_index, gradient, hessian, child_id, smaller_side):
    leaves = smaller_side.shape[0]
    features = bin_index.shape[1]
    target = 2 * jnp.arange(leaves, dtype=jnp.int32)[None, :] + smaller_side[None, :]
    chosen = child_id[:, None] == target
    nothing = jnp.zeros((), jnp.bfloat16)
    weights = jnp.concatenate(
        [
            jnp.where(chosen, gradient[:, None], nothing),
            jnp.where(chosen, hessian[:, None], nothing),
        ],
        axis=1,
    )
    levels = jnp.arange(BINS, dtype=jnp.int32)

    def one_feature(column):
        onehot = (column[:, None] == levels[None, :]).astype(jnp.bfloat16)
        product = lax.dot_general(
            weights, onehot, (((0,), (0,)), ((), ())), preferred_element_type=jnp.float32
        )
        return product.reshape(2, leaves, BINS).transpose(1, 0, 2).reshape(leaves, 2 * BINS)

    stacked = lax.map(one_feature, bin_index.T)
    owned = lax.psum_scatter(stacked, "dev", scatter_dimension=0, tiled=True)
    owned = lax.psum_scatter(owned, "group", scatter_dimension=1, tiled=True)
    hist_grad = owned[:, :, :BINS].transpose(1, 0, 2)
    hist_hess = owned[:, :, BINS:].transpose(1, 0, 2)
    best_gain = split_gains(hist_grad, hist_hess)
    child_best = lax.pmax(jnp.max(best_gain, axis=1), "dev")
    return (best_gain, child_best)


def kernel(
    groups, devs, leaves,
    bins_ref, grad_ref, hess_ref, child_ref, side_ref,
    done_ref,
    bins_v, side_v, grad_v, hess_v, child_v, values, bins_sem, small_sem,
    bins_t, weights, out, pair_in, a_in, b_in, c_in, d_in, e_in, f_out, f_in, near_in,
    gain_out, gain_in, best_in,
    pair_sem, a_sem, b_sem, c_sem, d_sem, e_sem, f_sem, near_sem, gain_sem, best_sem,
):
    rows, features = bins_ref.shape
    per_dev = features // devs
    own_features = per_dev // groups
    own_leaves = leaves // groups
    width = 2 * leaves
    slots = LANES // width
    quads = own_features // slots
    half = quads // 2
    planes = devs // 4
    last = planes - 1
    relayed = last - 1
    me_g = lax.axis_index("group")
    me_d = lax.axis_index("dev")
    me_c = lax.rem(me_d, 2)
    me_j = lax.div(me_d, 2)
    me_x = lax.rem(me_j, 2)
    me_z = lax.div(me_j, 2)
    barrier = pltpu.get_barrier_semaphore()
    step_rows = STEP_ROWS
    everyone = groups * devs

    def bins_copy(number):
        here = pl.ds(pl.multiple_of(number * step_rows, step_rows), step_rows)
        return pltpu.make_async_copy(bins_ref.at[here, :], bins_v.at[here, :], bins_sem.at[number])

    small = [
        pltpu.make_async_copy(source, place, small_sem.at[number])
        for number, (source, place) in enumerate(
            [(side_ref, side_v), (child_ref, child_v), (grad_ref, grad_v), (hess_ref, hess_v)]
        )
    ]
    for copy in small:
        copy.start()

    def start_bins(number, carry):
        bins_copy(number).start()
        return carry

    lax.fori_loop(0, rows // step_rows, start_bins, 0)

    def at(g, d):
        return {"group": g, "dev": d}

    def nth(step):
        other = lax.rem(me_g * devs + me_d + step, everyone)
        return at(lax.div(other, devs), lax.rem(other, devs))

    def greet(step, carry):
        pl.semaphore_signal(barrier, inc=1, device_id=nth(step), device_id_type=pl.DeviceIdType.MESH)
        return carry

    lax.fori_loop(1, everyone, greet, 0)

    pair_row = lax.broadcasted_iota(jnp.int32, (leaves, leaves), 0)
    pair_lane = lax.broadcasted_iota(jnp.int32, (leaves, leaves), 1)

    for copy in small:
        copy.wait()

    side = jnp.where(pair_lane == pair_row, side_v[...].astype(jnp.float32), 0.0)
    target = jnp.sum(side, axis=1, keepdims=True) + 2.0 * pair_row[:, :1].astype(jnp.float32)
    target = jnp.broadcast_to(target, (leaves, LANES)).astype(jnp.bfloat16)
    values[0] = grad_v[...].astype(jnp.float32)
    values[1] = hess_v[...].astype(jnp.float32)
    values[2] = child_v[...].astype(jnp.float32)
    no_weight = jnp.zeros((), jnp.bfloat16)

    def prepare(number, carry):
        here = pl.ds(pl.multiple_of(number * step_rows, step_rows), step_rows)
        for piece in range(step_rows // LANES):
            row = number * (step_rows // LANES) + piece
            there = pl.ds(pl.multiple_of(row * LANES, LANES), LANES)

            def spread(kind):
                return jnp.broadcast_to(values[kind, pl.ds(row, 1), :], (leaves, LANES)).astype(jnp.bfloat16)

            chosen = spread(2) == target
            for kind in range(2):
                value = jnp.where(chosen, spread(kind), no_weight)
                for s in range(slots):
                    start = s * width + kind * leaves
                    weights[start:start + leaves, there] = value
        return carry

    def turn_bins(number, carry):
        here = pl.ds(pl.multiple_of(number * step_rows, step_rows), step_rows)
        bins_copy(number).wait()
        bins_t[:, here] = bins_v[here, :].astype(jnp.float32).astype(jnp.bfloat16).T.astype(jnp.float32)
        return carry

    lax.fori_loop(0, rows // step_rows, prepare, 0)
    lax.fori_loop(0, rows // step_rows, turn_bins, 0)

    chunk = min(rows, KCHUNK)
    pack = 16
    level = lax.broadcasted_iota(jnp.int32, (pack, chunk), 0).astype(jnp.float32).astype(jnp.bfloat16)
    one = jnp.ones((), jnp.bfloat16)
    zero = jnp.zeros((), jnp.bfloat16)
    lane = lax.broadcasted_iota(jnp.int32, (BINS, LANES), 1)

    def block(d):
        base = pl.multiple_of(d * per_dev, per_dev)
        total = None
        for start in range(0, rows, chunk):
            parts = []
            levels = bins_t[pl.ds(base, per_dev), start:start + chunk]
            for f in range(per_dev):
                row = jnp.broadcast_to(levels[f:f + 1, :], (pack, chunk)).astype(jnp.bfloat16)
                for low in range(0, BINS, pack):
                    parts.append(jnp.where(row <= level + jnp.bfloat16(low), one, zero))
            below = jnp.concatenate(parts, axis=0)
            product = lax.dot_general(
                below, weights[:, start:start + chunk], (((1,), (1,)), ((), ())),
                preferred_element_type=jnp.float32,
            )
            total = product if total is None else total + product
        result = []
        for y in range(groups):
            for q in range(quads):
                piece = None
                for s in range(slots):
                    f = (y * quads + q) * slots + s
                    here = total[f * BINS:(f + 1) * BINS, :]
                    piece = here if piece is None else jnp.where(lane >= s * width, here, piece)
                result.append((y, q, piece))
        return result

    def remote(source, place, sem, index, device):
        return pltpu.make_async_remote_copy(
            src_ref=source, dst_ref=place, send_sem=sem.at[0, index], recv_sem=sem.at[1, index],
            device_id=device, device_id_type=pl.DeviceIdType.MESH,
        )

    def pick(index, choices):
        result = choices[-1]
        for number in range(len(choices) - 1):
            result = jnp.where(index == number, choices[number], result)
        return result

    def flipped(turn):
        result, bit = 0, 1
        while bit < planes:
            digit = lax.rem(lax.div(me_z, bit), 2)
            result = result + bit * (1 - digit if (turn // bit) % 2 else digit)
            bit *= 2
        return result

    planes_of = [flipped(last - k) for k in range(planes)]

    def plane(k):
        return planes_of[k] if isinstance(k, int) else pick(k, planes_of)

    def dev_of(k, dx, core):
        x = jnp.where(dx == 1, 1 - me_x, me_x)
        return (plane(k) * 2 + x) * 2 + core

    pair_dev = at(me_g, me_j * 2 + 1 - me_c)
    x_dev_d = (me_z * 2 + 1 - me_x) * 2 + me_c
    x_dev = at(me_g, x_dev_d)
    y_g = 1 - me_g
    y_dev = at(y_g, me_d)
    diag_dev = at(y_g, x_dev_d)

    def pair_copy(n):
        return remote(out.at[0, n], pair_in.at[n], pair_sem, n, pair_dev)

    first = slice(0, half)
    second = slice(half, quads)

    def a_copy(k):
        return remote(out.at[1, 2 * k + 1, first], a_in.at[k], a_sem, k, x_dev)

    def b_copy(k):
        return remote(out.at[1, 2 * k + 1, second, me_g], b_in.at[k], b_sem, k, x_dev)

    def c_copy(k):
        return remote(out.at[1, 2 * k + 1, second, y_g], c_in.at[k], c_sem, k, y_dev)

    def d_copy(k):
        return remote(out.at[1, 2 * k, second, y_g], d_in.at[k], d_sem, k, y_dev)

    def e_copy(k):
        return remote(out.at[1, 2 * k, first, y_g], e_in.at[k], e_sem, k, y_dev)

    def f_copy(k):
        d = (plane(k) * 2 + me_x) * 2 + me_c
        return remote(f_out.at[k], f_in.at[k], f_sem, k, at(me_g, d))

    def direct_copy(k, n):
        dx, y = ((1, y_g), (1, me_g), (0, y_g), (0, me_g))[n]
        d = dev_of(k, dx, me_c)
        return remote(out.at[1, 2 * k + dx, :, y], near_in.at[k - relayed, n], near_sem, (k - relayed) * 4 + n, at(y, d))

    def direct(k):
        return range(3 if k == last else 4)

    def do_b(k):
        c_copy(k).wait_recv()
        out[1, 2 * k + 1, second, me_g] = out[1, 2 * k + 1, second, me_g] + c_in[k]
        b_copy(k).start()

    def do_e(k):
        a_copy(k).wait_recv()
        out[1, 2 * k, first, y_g] = out[1, 2 * k, first, y_g] + a_in[k, :, y_g]
        e_copy(k).start()

    def do_f(k):
        b_copy(k).wait_recv()
        d_copy(k).wait_recv()
        f_out[k, second] = out[1, 2 * k, second, me_g] + b_in[k] + d_in[k]
        e_copy(k).wait_recv()
        f_out[k, first] = out[1, 2 * k, first, me_g] + a_in[k, :, me_g] + e_in[k]
        f_copy(k).start()

    steps = [(k, 1) for k in range(last)] + [(k, 0) for k in range(last)] + [(last, 1), (last, 0)]
    turns = len(steps)

    def group_of(step):
        k = pick(step, [a for a, _ in steps])
        dx = pick(step, [a for _, a in steps])
        return k, dx, 2 * k + dx

    def work(step, is_p):
        k, dx, n = group_of(step)
        role = jnp.where(is_p, 0, 1)
        for y, q, piece in block(dev_of(k, dx, jnp.where(is_p, 1 - me_c, me_c))):
            out[role, n, q, y] = piece

    def pass_on(step):
        k, dx, n = group_of(step)
        pair_copy(n).wait_recv()
        out[1, n] = out[1, n] + pair_in[n]

        @pl.when(k < relayed)
        def _():
            @pl.when(dx == 1)
            def _():
                a_copy(k).start()
                c_copy(k).start()

            @pl.when(dx == 0)
            def _():
                d_copy(k).start()
                do_e(k)
                do_b(k)

        @pl.when(k >= relayed)
        def _():
            @pl.when(dx == 1)
            def _():
                direct_copy(k, 0).start()
                direct_copy(k, 1).start()

            @pl.when(dx == 0)
            def _():
                direct_copy(k, 2).start()

                @pl.when(k < last)
                def _():
                    direct_copy(k, 3).start()

    def iteration(turn, carry):
        step = lax.div(turn, 2) * 2
        is_p = lax.rem(turn, 2) == 0
        work(step, is_p)
        work(step + 1, is_p)

        @pl.when(turn == 0)
        def _():
            pl.semaphore_wait(barrier, everyone - 1)

        @pl.when(is_p)
        def _():
            pair_copy(group_of(step)[2]).start()
            pair_copy(group_of(step + 1)[2]).start()

        @pl.when(jnp.logical_not(is_p))
        def _():
            for k in range(relayed - 1):
                @pl.when(turn == turns - 1 - 2 * (relayed - 1 - k))
                def _():
                    do_f(k)

            pass_on(step)
            pass_on(step + 1)

        return carry

    lax.fori_loop(0, turns - 2, iteration, 0)

    def closing(slot, carry):
        step = turns - 2 + lax.div(slot, 2)
        is_p = lax.rem(slot, 2) == 0
        work(step, is_p)

        @pl.when(is_p)
        def _():
            pair_copy(group_of(step)[2]).start()

        @pl.when(jnp.logical_not(is_p))
        def _():
            pass_on(step)

        @pl.when(slot == 2)
        def _():
            do_f(relayed - 1)

        return carry

    lax.fori_loop(0, 4, closing, 0)

    hist = out[1, 2 * last, :, me_g]
    for k in range(relayed):
        f_copy(k).wait_recv()
        hist = hist + f_in[k]
    for k in range(relayed, planes):
        for number in direct(k):
            direct_copy(k, number).wait_recv()
            hist = hist + near_in[k - relayed, number]

    usable = lax.rem(lane, width) < leaves
    keep = lax.broadcasted_iota(jnp.int32, (BINS, LANES), 0) < BINS - 1
    lane8 = lax.broadcasted_iota(jnp.int32, (8, LANES), 1)
    row8 = lax.broadcasted_iota(jnp.int32, (8, LANES), 0)
    tile = jnp.full((8, LANES), -jnp.inf, jnp.float32)
    for q in range(quads):
        left_grad = hist[q]
        left_hess = jnp.where(usable, pltpu.roll(left_grad, LANES - leaves, 1), 0.0)
        total_grad, total_hess = left_grad[BINS - 1:, :], left_hess[BINS - 1:, :]
        right_grad = total_grad - left_grad
        value = left_grad * left_grad / (left_hess + reg_lambda)
        value = value + right_grad * right_grad / (total_hess - left_hess + reg_lambda)
        value = value - total_grad * total_grad / (total_hess + reg_lambda)
        value = jnp.where(keep, value, -jnp.inf)
        best = jnp.broadcast_to(jnp.max(value, axis=0, keepdims=True), (8, LANES))
        for s in range(slots):
            moved = pltpu.roll(best, LANES - s * width, 1) if s else best
            tile = jnp.where(row8 == q * slots + s, moved, tile)
    top = jnp.max(tile, axis=0, keepdims=True)
    tile = jnp.where(row8 == 7, top, tile)
    gain_out[...] = tile

    gain_copy = remote(gain_out, gain_in, gain_sem, 0, y_dev)

    def best_copy(step):
        return remote(gain_out.at[pl.ds(7, 1)], best_in.at[step], best_sem, step, nth(step))

    for step in range(1, everyone):
        if step != devs:
            best_copy(step).start()
    gain_copy.start()
    for n in range(2 * planes):
        pair_copy(n).wait_send()
    for k in range(relayed):
        for make in (a_copy, b_copy, c_copy, d_copy, e_copy, f_copy):
            make(k).wait_send()
    for k in range(relayed, planes):
        for number in direct(k):
            direct_copy(k, number).wait_send()
    gain_copy.wait_recv()
    other = gain_in[...]
    top = jnp.maximum(top, other[7:8, :])
    low_tile = jnp.where(me_g == 0, tile, other)
    high_tile = jnp.where(me_g == 0, other, tile)
    gain = jnp.where(row8 < own_features, low_tile, pltpu.roll(high_tile, own_features, 0))
    done_ref[0] = jnp.where(me_g == 0, gain, pltpu.roll(gain, LANES - own_leaves, 1))
    for step in range(1, everyone):
        if step != devs:
            best_copy(step).wait_recv()
            top = jnp.maximum(top, best_in[step])
    top = jnp.broadcast_to(top, (8, LANES))
    done_ref[1] = jnp.where(me_g == 0, top, pltpu.roll(top, LANES - own_leaves, 1))
    gain_copy.wait_send()
    for step in range(1, everyone):
        if step != devs:
            best_copy(step).wait_send()


def finish(done_ref, gain_ref, best_ref):
    gain_ref[...] = done_ref[0, :gain_ref.shape[0], :gain_ref.shape[1]]
    best_ref[...] = done_ref[1, 0, :best_ref.shape[0]]


def kernel_body(groups, devs, bin_index, gradient, hessian, child_id, smaller_side):
    rows, features = bin_index.shape
    leaves = smaller_side.shape[0]
    per_dev = features // devs
    own_features = per_dev // groups
    own_leaves = leaves // groups
    slots = LANES // (2 * leaves)
    quads = own_features // slots
    half = quads // 2
    planes = devs // 4
    relayed = planes - 2
    everyone = groups * devs
    vmem = pl.BlockSpec(memory_space=pltpu.VMEM)
    hbm = pl.BlockSpec(memory_space=pltpu.HBM)

    def floats(*shape):
        return pltpu.VMEM(shape + (BINS, LANES), jnp.float32)

    def sems(number):
        return pltpu.SemaphoreType.DMA((2, number))

    done = pl.pallas_call(
        functools.partial(kernel, groups, devs, leaves),
        out_shape=jax.ShapeDtypeStruct((2, 8, LANES), jnp.float32),
        in_specs=[hbm] * 5,
        out_specs=vmem,
        scratch_shapes=[
            pltpu.VMEM((rows, features), jnp.int32),
            pltpu.VMEM((1, leaves), jnp.int32),
            pltpu.VMEM((rows // LANES, LANES), jnp.bfloat16),
            pltpu.VMEM((rows // LANES, LANES), jnp.bfloat16),
            pltpu.VMEM((rows // LANES, LANES), jnp.int32),
            pltpu.VMEM((3, rows // LANES, LANES), jnp.float32),
            pltpu.SemaphoreType.DMA((rows // STEP_ROWS,)),
            pltpu.SemaphoreType.DMA((4,)),
            pltpu.VMEM((features, rows), jnp.float32),
            pltpu.VMEM((LANES, rows), jnp.bfloat16),
            floats(2, 2 * planes, quads, groups),
            floats(2 * planes, quads, groups),
            floats(relayed, half, groups),
            floats(relayed, half),
            floats(relayed, half),
            floats(relayed, half),
            floats(relayed, half),
            floats(relayed, quads),
            floats(relayed, quads),
            floats(2, 4, quads),
            pltpu.VMEM((8, LANES), jnp.float32),
            pltpu.VMEM((8, LANES), jnp.float32),
            pltpu.VMEM((everyone, 1, LANES), jnp.float32),
            sems(2 * planes),
            sems(relayed),
            sems(relayed),
            sems(relayed),
            sems(relayed),
            sems(relayed),
            sems(relayed),
            sems(8),
            sems(1),
            sems(everyone),
        ],
        compiler_params=pltpu.CompilerParams(
            collective_id=0, has_side_effects=True, vmem_limit_bytes=63 * 1024 * 1024
        ),
    )(
        bin_index, gradient.reshape(rows // LANES, LANES), hessian.reshape(rows // LANES, LANES),
        child_id.reshape(rows // LANES, LANES), smaller_side.reshape(1, leaves),
    )
    gain, best = pl.pallas_call(
        finish,
        out_shape=(
            jax.ShapeDtypeStruct((per_dev, own_leaves), jnp.float32),
            jax.ShapeDtypeStruct((own_leaves,), jnp.float32),
        ),
        in_specs=[vmem],
        out_specs=(vmem, vmem),
    )(done)
    return (gain.T, best)


def fits(groups, devs, leaves, features, rows):
    planes = devs // 4
    if groups != 2 or devs % 4 or planes != 4 or leaves != 32:
        return False
    return features == 8 * devs and rows % KCHUNK == 0 and rows % STEP_ROWS == 0


def solution(mesh):
    in_specs = (
        P(("group", "dev"), None),
        P(("group", "dev")),
        P(("group", "dev")),
        P(("group", "dev")),
        P(),
    )
    out_specs = (P("group", "dev"), P("group"))
    groups, devs = mesh.shape["group"], mesh.shape["dev"]

    def body(bin_index, gradient, hessian, child_id, smaller_side):
        rows, features = bin_index.shape
        args = (bin_index, gradient, hessian, child_id, smaller_side)
        if fits(groups, devs, smaller_side.shape[0], features, rows):
            return kernel_body(groups, devs, *args)
        return plain_body(*args)

    return jax.shard_map(body, mesh=mesh, in_specs=in_specs, out_specs=out_specs, check_vma=False)
```
